512 devices in a mesh: group: 16 (over z, core), tensor: 32 (over y, x).
Axes of the slice: x: 4, y: 8, z: 8, core: 2. Of those that a mesh axis runs over, the one named last changes fastest.
Arguments:
- key_value_cache: bfloat16 [1024, 1024, 256], P(('group', 'tensor')), may hold values from -8 to 8
- queries: bfloat16 [128, 48, 128], P('group'), may hold values from -200 to 200
- fresh_key_value: bfloat16 [128, 8, 256], P('group'), may hold values from -6 to 6
- lengths: int32 [128], P('group'), may hold values from 2 to 1023
- residual: bfloat16 [128, 6144], P('group'), may hold values from -100 to 100
- norm_gain: float32 [6144], replicated, may hold values from 0.1 to 1.9
- router_weight: bfloat16 [6144, 8], replicated, may hold values from -0.078125 to 0.078125
- routing: int32 [128, 2], P('group'), may hold values from 0 to 7, all different within a row
- expert_gate: bfloat16 [8, 6144, 8192], P(None, 'group', 'tensor'), may hold values from -0.078125 to 0.078125
- expert_up: bfloat16 [8, 6144, 8192], P(None, 'group', 'tensor'), may hold values from -0.078125 to 0.078125
Outputs:
- updated: bfloat16 [128, 6144], P('group')
- expert_hidden: bfloat16 [128, 2, 8192], P('group', None, 'tensor')
- new_cache: bfloat16 [128, 8, 1024, 256], P('group', None, 'tensor')
The draws below stay inside these ranges and needn't reach their ends.
Inputs may be any that keep to these rules, and one draw needn't show every extreme that they name: Slot lengths[s] of sequence s receives its new token. `routing`: A token's two experts differ.
All inputs are finite; a program needn't handle non-finite values.
Results may differ from the reference program's by a relative error of at most 0.028.
Values may be sent and summed in bfloat16 or wider, within the bound.
A program may use at most 64 MiB of HBM per device.

```python
import math
import jax
import jax.numpy as jnp
from jax import lax

D = 6144
QUERY_HEADS = 48
KEY_VALUE_HEADS = 8
HEAD_DIM = 128
EXPERTS = 8
TOPK = 2
FF_WIN = 8192
CONTEXT_SLOTS = 1024
SEQUENCE_TOTAL = 128


def starting_cache(key):
    cache_random_key = jax.random.fold_in(key, 7)
    return jnp.clip(jax.random.normal(cache_random_key, (SEQUENCE_TOTAL * KEY_VALUE_HEADS, CONTEXT_SLOTS, 2 * HEAD_DIM), jnp.float32), -6.0, 6.0)


def draw_key_value_cache(key, part):
    cache_layout_grid = starting_cache(key)
    return cache_layout_grid.astype(jnp.bfloat16)


def draw_queries(key, part):
    query_group_width = QUERY_HEADS // KEY_VALUE_HEADS
    query_vectors = jnp.clip(jax.random.normal(jax.random.fold_in(key, 21), (SEQUENCE_TOTAL, KEY_VALUE_HEADS, query_group_width, HEAD_DIM), jnp.float32), -4.0, 4.0)
    return query_vectors.reshape(SEQUENCE_TOTAL, QUERY_HEADS, HEAD_DIM).astype(jnp.bfloat16)


def draw_residual(key, part):
    base_key = jax.random.fold_in(key, 31)
    row_key = jax.random.fold_in(key, 32)
    column_key = jax.random.fold_in(key, 33)
    values = jnp.clip(jax.random.normal(base_key, (SEQUENCE_TOTAL, D), jnp.float32), -4.0, 4.0)
    row_scale = jnp.exp(jax.random.uniform(row_key, (SEQUENCE_TOTAL, 1), jnp.float32, jnp.log(0.4), jnp.log(4.0)))
    column_scale = jnp.exp(jax.random.uniform(column_key, (1, D), jnp.float32, jnp.log(0.4), jnp.log(4.0)))
    return (values * row_scale * column_scale).astype(jnp.bfloat16)


def touch_ends(values, rng, least, high):
    dims = values.shape
    spot = [jax.random.randint(jax.random.fold_in(rng, axis), (), 0, dims[axis]) for axis in range(len(dims))]
    values = values.at[tuple(spot)].set(least)
    longest = dims.index(max(dims))
    spot[longest] = (spot[longest] + 1) % dims[longest]
    return values.at[tuple(spot)].set(high)


def shard_levels(rng, shape, pieces, smallest, high):
    level, own = 1.0, jax.random.fold_in(rng, 6)
    for position, shards_of in pieces:
        heights = jnp.exp(jax.random.uniform(jax.random.fold_in(own, position), (shards_of,), jnp.float32, smallest / len(pieces), high / len(pieces)))
        level = level * jnp.repeat(heights, shape[position] // shards_of).reshape([-1 if axis == position else 1 for axis in range(len(shape))])
    return level


def picks_of(key, rows, amount, top, lift):
    sequence = jax.random.permutation(jax.random.fold_in(key, 1), amount)
    boost = sequence
    for power in range(3):
        boost = boost * boost // amount
    boost = boost * lift // amount
    tickets = jax.random.randint(jax.random.fold_in(key, 2), (rows, amount), 0, 4096) + boost
    holders = jax.random.permutation(jax.random.fold_in(key, 3), rows)[jnp.arange(amount) % rows]
    tickets = jnp.where(jnp.arange(rows)[:, None] == holders[None, :], 1 << 14, tickets)
    merit = tickets * amount + jnp.arange(amount)
    return lax.top_k(merit.astype(jnp.int32), top)[1].astype(jnp.int32)


def scatter_about(key, extent, scale, limit, shards=(), kind=jnp.bfloat16):
    loudness = shard_levels(key, extent, shards, -0.22, 0.18) if shards else 1.0
    values = jax.random.normal(key, extent, jnp.float32) * scale * loudness
    return jnp.minimum(jnp.maximum(values, -limit), limit).astype(kind)


def setup_inputs(seed: int = 0) -> dict:
    key_of = jax.random.split(jax.random.key(seed), 11)
    return {
        "key_value_cache": draw_key_value_cache(jax.random.fold_in(key_of[10], 71), 0),
        "queries": draw_queries(jax.random.fold_in(key_of[10], 71), 0),
        "fresh_key_value": scatter_about(key_of[2], (SEQUENCE_TOTAL, KEY_VALUE_HEADS, 2 * HEAD_DIM), 1.0, 6.0, ((0, 16),)),
        "lengths": touch_ends(jax.random.randint(key_of[3], (SEQUENCE_TOTAL,), 2, CONTEXT_SLOTS), jax.random.fold_in(key_of[3], 1), 2, CONTEXT_SLOTS - 1).astype(jnp.int32),
        "residual": draw_residual(jax.random.fold_in(key_of[10], 71), 0),
        "norm_gain": jnp.clip(1.0 + 0.18 * jax.random.normal(key_of[5], (D,), jnp.float32), 0.1, 1.9),
        "router_weight": scatter_about(key_of[6], (D, EXPERTS), D ** -0.5, 0.078125),
        "routing": picks_of(key_of[7], SEQUENCE_TOTAL, EXPERTS, TOPK, 2048),
        "expert_gate": scatter_about(key_of[8], (EXPERTS, D, FF_WIN), D ** -0.5, 0.078125, ((1, 16), (2, 32))),
        "expert_up": scatter_about(key_of[9], (EXPERTS, D, FF_WIN), D ** -0.5, 0.078125, ((1, 16), (2, 32))),
    }


def reference(key_value_cache, queries, fresh_key_value, lengths, residual, norm_gain, router_weight, routing, expert_gate, expert_up):
    query_group_width = QUERY_HEADS // KEY_VALUE_HEADS
    cache_layout_grid = key_value_cache.reshape(SEQUENCE_TOTAL, KEY_VALUE_HEADS, CONTEXT_SLOTS, 2 * HEAD_DIM)
    key_rows = cache_layout_grid[..., :HEAD_DIM].astype(jnp.float32)
    value_rows = cache_layout_grid[..., HEAD_DIM:].astype(jnp.float32)
    query_vectors = queries.reshape(SEQUENCE_TOTAL, KEY_VALUE_HEADS, query_group_width, HEAD_DIM).astype(jnp.float32)
    score_scale = 1.0 / math.sqrt(HEAD_DIM)
    scores = jnp.einsum('sngd,sntd->sngt', query_vectors, key_rows, precision=lax.Precision.HIGHEST) * score_scale
    own_key = fresh_key_value[..., :HEAD_DIM].astype(jnp.float32)
    own_value = fresh_key_value[..., HEAD_DIM:].astype(jnp.float32)
    own_score = jnp.einsum('sngd,snd->sng', query_vectors, own_key, precision=lax.Precision.HIGHEST) * score_scale
    visible = jnp.arange(CONTEXT_SLOTS, dtype=jnp.int32)[None, None, None, :] < lengths[:, None, None, None]
    peak = jnp.maximum(lax.optimization_barrier(jnp.max(jnp.where(visible, scores, -jnp.inf), -1)), own_score)
    attention_weights = jnp.where(visible, jnp.exp(scores - peak[..., None]), 0.0)
    own_weight = jnp.exp(own_score - peak)
    denominator = lax.optimization_barrier(jnp.sum(attention_weights, -1)) + own_weight
    rounded = lax.optimization_barrier(attention_weights.astype(jnp.bfloat16)).astype(jnp.float32)
    own_rounded = lax.optimization_barrier(own_weight.astype(jnp.bfloat16)).astype(jnp.float32)
    weighted = jnp.einsum('sngt,sntd->sngd', rounded, value_rows, precision=lax.Precision.HIGHEST)
    weighted = weighted + own_rounded[..., None] * own_value[:, :, None, :]
    attention = (weighted / denominator[..., None]).reshape(SEQUENCE_TOTAL, D)
    updated = (residual.astype(jnp.float32) + attention).astype(jnp.bfloat16)
    stream = updated.astype(jnp.float32)
    normed = (stream * lax.rsqrt(lax.optimization_barrier(jnp.mean(stream * stream, -1, keepdims=True)) + 1e-05) * norm_gain).astype(jnp.bfloat16)
    logits = jnp.dot(normed, router_weight, preferred_element_type=jnp.float32)
    chosen_mask = routing[:, :, None] == jnp.arange(EXPERTS, dtype=jnp.int32)[None, None, :]
    chosen_logits = lax.optimization_barrier(jnp.sum(jnp.where(chosen_mask, logits[:, None, :], 0.0), -1))
    gate_weights = jax.nn.sigmoid(chosen_logits - chosen_logits[:, ::-1])

    def expert_pass(weight_pair):
        gate_part = jnp.dot(normed, weight_pair[0], preferred_element_type=jnp.float32)
        up_part = jnp.dot(normed, weight_pair[1], preferred_element_type=jnp.float32)
        return jnp.stack((gate_part, up_part), 1)
    every_expert = lax.map(expert_pass, (expert_gate, expert_up))
    every_expert = jnp.transpose(every_expert, (1, 0, 2, 3))
    picked = lax.optimization_barrier(jnp.sum(jnp.where(chosen_mask[:, :, :, None, None], every_expert[:, None], 0.0), 2))
    expert_hidden = (gate_weights[:, :, None] * jax.nn.silu(picked[:, :, 0]) * picked[:, :, 1]).astype(jnp.bfloat16)
    new_slot = jnp.arange(CONTEXT_SLOTS, dtype=jnp.int32)[None, None, :, None] == lengths[:, None, None, None]
    new_cache = jnp.where(new_slot, fresh_key_value[:, :, None, :], cache_layout_grid)
    return (updated, expert_hidden, new_cache)
```

```python
import functools
import math

import jax
import jax.numpy as jnp
from jax import lax
from jax.experimental import pallas as pl
from jax.experimental.pallas import tpu as pltpu
from jax.sharding import PartitionSpec as P

MESH = pl.DeviceIdType.MESH
LANES = 128
ROWS = 16
NT = (((1,), (1,)), ((), ()))


def kernel(
    dims,
    lengths,
    routing,
    cache_hbm,
    queries_hbm,
    fresh_hbm,
    residual_hbm,
    gain_hbm,
    router_hbm,
    gate_hbm,
    up_hbm,
    updated_out,
    hidden_out,
    cache_out,
    cache,
    queries,
    fresh,
    residual,
    gain,
    router,
    gate_w,
    up_w,
    residual_rows,
    stream,
    stream_rows,
    tiles,
    normed,
    columns,
    tokens,
    routes,
    gate_all,
    up_all,
    partial,
    arrived,
    load_sem,
    local_sem,
    stream_send,
    stream_recv,
    cache_send,
    cache_recv,
    route_send,
    route_recv,
    column_send,
    column_recv,
    sum_send,
    sum_recv,
):
    groups, tensors, span = dims
    mine = lax.axis_index("group")
    rank = lax.axis_index("tensor")
    pairs, slots, width = cache.shape
    head = width // 2
    seqs, cols = updated_out.shape
    per_seq = tensors // seqs
    seq = rank // per_seq
    part = lax.rem(rank, per_seq)
    heads = cols // per_seq // head
    share = heads // pairs
    blocks = cols // LANES
    own_blocks = blocks // groups
    experts = gate_w.shape[0]
    hidden = gate_w.shape[2]

    def tensor_peer(i):
        return lax.rem(rank + i, tensors)

    def group_peer(i):
        return lax.rem(mine + i, groups)

    def cache_copy(to, slot):
        return pltpu.make_async_remote_copy(
            src_ref=cache.at[:, pl.ds(pl.multiple_of(to * span, span), span), :],
            dst_ref=cache_out.at[pl.ds(slot * pairs, pairs)],
            send_sem=cache_send.at[to],
            recv_sem=cache_recv.at[slot],
            device_id={"tensor": to},
            device_id_type=MESH,
        )

    def stream_copy(to, slot):
        return pltpu.make_async_remote_copy(
            src_ref=stream.at[slot],
            dst_ref=stream.at[slot],
            send_sem=stream_send.at[to],
            recv_sem=stream_recv.at[slot],
            device_id={"tensor": to},
            device_id_type=MESH,
        )

    def route_copy(to, slot):
        return pltpu.make_async_remote_copy(
            src_ref=routes.at[slot],
            dst_ref=routes.at[slot],
            send_sem=route_send.at[to],
            recv_sem=route_recv.at[slot],
            device_id={"group": to},
            device_id_type=MESH,
        )

    def column_copy(to, slot):
        return pltpu.make_async_remote_copy(
            src_ref=normed.at[pl.ds(to * own_blocks, own_blocks)],
            dst_ref=columns.at[slot],
            send_sem=column_send.at[to],
            recv_sem=column_recv.at[slot],
            device_id={"group": to},
            device_id_type=MESH,
        )

    def sum_copy(to, slot):
        return pltpu.make_async_remote_copy(
            src_ref=partial.at[to],
            dst_ref=arrived.at[slot],
            send_sem=sum_send.at[to],
            recv_sem=sum_recv.at[slot],
            device_id={"group": to},
            device_id_type=MESH,
        )

    def each(count, step):
        def go(i, carry):
            step(i)
            return carry

        lax.fori_loop(1, count, go, 0)

    barrier = pltpu.get_barrier_semaphore()
    each(
        tensors,
        lambda i: pl.semaphore_signal(
            barrier, inc=1, device_id={"tensor": tensor_peer(i)}, device_id_type=MESH
        ),
    )
    each(
        groups,
        lambda i: pl.semaphore_signal(
            barrier, inc=1, device_id={"group": group_peer(i)}, device_id_type=MESH
        ),
    )

    loads = [
        pltpu.make_async_copy(source, target, load_sem.at[k])
        for k, (source, target) in enumerate(
            (
                (cache_hbm, cache),
                (queries_hbm.at[seq], queries),
                (fresh_hbm.at[seq], fresh),
                (residual_hbm, residual),
                (gain_hbm, gain),
                (router_hbm, router),
                (gate_hbm, gate_w),
                (up_hbm, up_w),
            )
        )
    ]
    for load in loads:
        load.start()
    for load in loads[:4]:
        load.wait()

    length = lengths[seq]
    fresh_rows = fresh[...].astype(jnp.float32)
    row_id = lax.broadcasted_iota(jnp.int32, fresh_rows.shape, 0)
    chunk = 128
    for p in range(pairs):
        own_row = jnp.sum(
            jnp.where(row_id == part * pairs + p, fresh_rows, 0.0), axis=0, keepdims=True
        )

        def place(c, carry, p=p, own_row=own_row):
            at = pl.ds(pl.multiple_of(c * chunk, chunk), chunk)
            slot_id = lax.broadcasted_iota(jnp.int32, (chunk, width), 0) + c * chunk
            cache[p, at, :] = jnp.where(
                slot_id == length, own_row, cache[p, at, :].astype(jnp.float32)
            ).astype(jnp.bfloat16)
            return carry

        lax.fori_loop(0, slots // chunk, place, 0)

    pick = (
        lax.broadcasted_iota(jnp.int32, (ROWS, queries.shape[0]), 1)
        == lax.broadcasted_iota(jnp.int32, (ROWS, queries.shape[0]), 0) + part * heads
    )
    own_queries = jnp.dot(
        pick.astype(jnp.float32).astype(jnp.bfloat16),
        queries[...],
        preferred_element_type=jnp.float32,
    ).astype(jnp.bfloat16)
    visible = lax.broadcasted_iota(jnp.int32, (ROWS, slots), 1) <= length
    out_row = lax.broadcasted_iota(jnp.int32, (ROWS, head), 0)
    attention = None
    for p in range(pairs):
        scores = lax.dot_general(
            own_queries, cache[p, :, :head], NT, preferred_element_type=jnp.float32
        ) * (1.0 / math.sqrt(head))
        scores = jnp.where(visible, scores, -1e30)
        peak = jnp.max(scores, axis=1, keepdims=True)
        weights = jnp.where(visible, jnp.exp(scores - peak), 0.0)
        denominator = jnp.sum(weights, axis=1, keepdims=True)
        weighted = jnp.dot(
            weights.astype(jnp.bfloat16), cache[p, :, head:], preferred_element_type=jnp.float32
        )
        result = weighted / denominator
        attention = result if p == 0 else jnp.where(out_row < p * share, attention, result)

    residual_rows[...] = jnp.zeros_like(residual_rows)
    for c in range(heads):
        at = pl.ds(pl.multiple_of(part * heads * LANES + c * LANES, LANES), LANES)
        residual_rows[c * seqs : (c + 1) * seqs, :] = residual[:, at].astype(jnp.float32)
    own_residual = residual_rows[pl.ds(seq, ROWS, stride=seqs), :]
    stream[rank] = (own_residual + attention).astype(jnp.bfloat16)

    sublane = lax.broadcasted_iota(jnp.int32, (seqs, LANES), 0)
    for k in range(routing.shape[0]):
        value = jnp.zeros((seqs, LANES), jnp.int32)
        for s in range(seqs):
            value = jnp.where(sublane == s, routing[k, s], value)
        routes[mine, k] = value

    pl.semaphore_wait(barrier, tensors + groups - 2)
    each(tensors, lambda i: stream_copy(tensor_peer(i), rank).start())
    each(groups, lambda i: route_copy(group_peer(i), mine).start())
    keep = pltpu.make_async_copy(
        cache.at[:, pl.ds(pl.multiple_of(rank * span, span), span), :],
        cache_out.at[pl.ds(rank * pairs, pairs)],
        local_sem,
    )
    keep.start()
    each(tensors, lambda i: cache_copy(tensor_peer(i), rank).start())
    for load in loads[4:]:
        load.wait()
    each(tensors, lambda i: stream_copy(rank, tensor_peer(i)).wait_recv())

    for k in range(tensors):
        stream_rows[k * ROWS : (k + 1) * ROWS, :] = stream[k].astype(jnp.float32)
    total = jnp.zeros((seqs, LANES), jnp.float32)
    for c in range(blocks):
        start = c // heads * ROWS + c % heads
        tile = stream_rows[pl.ds(start, seqs, stride=per_seq * ROWS), :]
        tiles[c] = tile
        total = total + tile * tile
        updated_out[:, c * LANES : (c + 1) * LANES] = tile.astype(jnp.bfloat16)
    scale = lax.rsqrt(jnp.sum(total, axis=1, keepdims=True) / cols + 1e-05)
    for c in range(blocks):
        normed[c] = (tiles[c] * scale * gain[c : c + 1, :]).astype(jnp.bfloat16)
    each(groups, lambda i: column_copy(group_peer(i), mine).start())
    columns[mine] = normed[pl.ds(mine * own_blocks, own_blocks)]

    logits = jnp.zeros((seqs, experts), jnp.float32)
    for c in range(blocks):
        logits = logits + lax.dot_general(
            normed[c],
            router[:, c * LANES : (c + 1) * LANES],
            NT,
            preferred_element_type=jnp.float32,
        )
    expert_id = lax.broadcasted_iota(jnp.int32, (seqs, experts), 1)
    chosen = [
        jnp.sum(
            jnp.where(routes[mine, k][:, :1] == expert_id, logits, 0.0), axis=1, keepdims=True
        )
        for k in range(2)
    ]
    gate_weights = [
        1.0 / (1.0 + jnp.exp(chosen[1] - chosen[0])),
        1.0 / (1.0 + jnp.exp(chosen[0] - chosen[1])),
    ]

    each(groups, lambda i: route_copy(mine, group_peer(i)).wait_recv())
    each(groups, lambda i: column_copy(mine, group_peer(i)).wait_recv())
    for c in range(own_blocks):
        tokens[:, c * LANES : (c + 1) * LANES] = (
            columns[:, c].astype(jnp.float32).reshape(groups * seqs, LANES).astype(jnp.bfloat16)
        )

    def products(e, carry):
        gate_all[e] = jnp.dot(tokens[...], gate_w[e], preferred_element_type=jnp.float32)
        up_all[e] = jnp.dot(tokens[...], up_w[e], preferred_element_type=jnp.float32)
        return carry

    lax.fori_loop(0, experts, products, 0)

    def choose(to):
        at = pl.ds(pl.multiple_of(to * seqs, seqs), seqs)
        for k in range(2):
            route = routes[to, k]
            route = jnp.concatenate([route] * (hidden // LANES), axis=1)
            for q, source in enumerate((gate_all, up_all)):
                value = source[0, at, :]
                for e in range(1, experts):
                    value = jnp.where(route == e, source[e, at, :], value)
                partial[to, 2 * k + q] = value.astype(jnp.bfloat16)

    def choose_and_send(i):
        choose(group_peer(i))

        @pl.when(i > 1)
        def _():
            sum_copy(group_peer(i - 1), mine).start()

    each(groups, choose_and_send)
    choose(mine)
    sum_copy(group_peer(groups - 1), mine).start()
    arrived[mine] = partial[mine]
    each(groups, lambda i: sum_copy(mine, group_peer(i)).wait_recv())

    for k in range(2):
        sums = []
        for q in range(2):
            value = arrived[0, 2 * k + q].astype(jnp.float32)
            for s in range(1, groups):
                value = value + arrived[s, 2 * k + q].astype(jnp.float32)
            sums.append(value)
        silu = sums[0] / (1.0 + jnp.exp(-sums[0]))
        hidden_out[k] = (gate_weights[k] * silu * sums[1]).astype(jnp.bfloat16)

    each(groups, lambda i: route_copy(group_peer(i), mine).wait_send())
    each(groups, lambda i: column_copy(group_peer(i), mine).wait_send())
    each(groups, lambda i: sum_copy(group_peer(i), mine).wait_send())
    each(tensors, lambda i: stream_copy(tensor_peer(i), rank).wait_send())
    each(tensors, lambda i: cache_copy(tensor_peer(i), rank).wait_send())
    each(tensors, lambda i: cache_copy(rank, tensor_peer(i)).wait_recv())
    keep.wait()


def body(
    groups,
    tensors,
    key_value_cache,
    queries,
    fresh_key_value,
    lengths,
    residual,
    norm_gain,
    router_weight,
    routing,
    expert_gate,
    expert_up,
):
    pairs, slots, width = key_value_cache.shape
    seqs, q_heads, head = queries.shape
    kv_heads = fresh_key_value.shape[1]
    cols = residual.shape[1]
    experts, own_cols, hidden = expert_gate.shape
    span = slots // tensors
    bf16, f32, i32 = jnp.bfloat16, jnp.float32, jnp.int32
    dma = pltpu.SemaphoreType.DMA
    hbm = pl.BlockSpec(memory_space=pltpu.HBM)
    vmem = pl.BlockSpec(memory_space=pltpu.VMEM)
    smem = pl.BlockSpec(memory_space=pltpu.SMEM)
    updated, hidden_units, new_cache = pl.pallas_call(
        functools.partial(kernel, (groups, tensors, span)),
        out_shape=(
            jax.ShapeDtypeStruct((seqs, cols), bf16),
            jax.ShapeDtypeStruct((2, seqs, hidden), bf16),
            jax.ShapeDtypeStruct((seqs * kv_heads, span, width), bf16),
        ),
        in_specs=[smem] * 2 + [hbm] * 8,
        out_specs=(vmem, vmem, hbm),
        scratch_shapes=[
            pltpu.VMEM((pairs, slots, width), bf16),
            pltpu.VMEM((q_heads, head), bf16),
            pltpu.VMEM((kv_heads, width), bf16),
            pltpu.VMEM((seqs, cols), bf16),
            pltpu.VMEM((cols // LANES, LANES), f32),
            pltpu.VMEM((experts, cols), bf16),
            pltpu.VMEM(expert_gate.shape, bf16),
            pltpu.VMEM(expert_up.shape, bf16),
            pltpu.VMEM((ROWS * seqs, LANES), f32),
            pltpu.VMEM((tensors, ROWS, LANES), bf16),
            pltpu.VMEM((tensors * ROWS, LANES), f32),
            pltpu.VMEM((cols // LANES, seqs, LANES), f32),
            pltpu.VMEM((cols // LANES, seqs, LANES), bf16),
            pltpu.VMEM((groups, own_cols // LANES, seqs, LANES), bf16),
            pltpu.VMEM((groups * seqs, own_cols), bf16),
            pltpu.VMEM((groups, 2, seqs, LANES), i32),
            pltpu.VMEM((experts, groups * seqs, hidden), f32),
            pltpu.VMEM((experts, groups * seqs, hidden), f32),
            pltpu.VMEM((groups, 4, seqs, hidden), bf16),
            pltpu.VMEM((groups, 4, seqs, hidden), bf16),
            dma((8,)),
            dma(()),
            dma((tensors,)),
            dma((tensors,)),
            dma((tensors,)),
            dma((tensors,)),
            dma((groups,)),
            dma((groups,)),
            dma((groups,)),
            dma((groups,)),
            dma((groups,)),
            dma((groups,)),
        ],
        compiler_params=pltpu.CompilerParams(collective_id=0, has_side_effects=True),
    )(
        lengths,
        routing.T,
        key_value_cache,
        queries,
        fresh_key_value,
        residual,
        norm_gain.reshape(cols // LANES, LANES),
        router_weight.T,
        expert_gate,
        expert_up,
    )
    return (
        updated,
        jnp.swapaxes(hidden_units, 0, 1),
        new_cache.reshape(seqs, kv_heads, span, width),
    )


def solution(mesh):
    in_specs = (
        P(("group", "tensor"), None, None),
        P("group", None, None),
        P("group", None, None),
        P("group"),
        P("group", None),
        P(),
        P(),
        P("group", None),
        P(None, "group", "tensor"),
        P(None, "group", "tensor"),
    )
    out_specs = (P("group", None), P("group", None, "tensor"), P("group", None, "tensor", None))
    return jax.shard_map(
        functools.partial(body, mesh.shape["group"], mesh.shape["tensor"]),
        mesh=mesh,
        in_specs=in_specs,
        out_specs=out_specs,
        check_vma=False,
    )
```

```python
import functools
import math

import jax
import jax.numpy as jnp
from jax import lax
from jax.experimental import pallas as pl
from jax.experimental.pallas import tpu as pltpu
from jax.sharding import PartitionSpec as P

MESH = pl.DeviceIdType.MESH
LANES = 128
ROWS = 16
NT = (((1,), (1,)), ((), ()))


def kernel(
    dims,
    lengths_hbm,
    routing_hbm,
    cache_hbm,
    queries_hbm,
    fresh_hbm,
    residual_hbm,
    gain_hbm,
    router_hbm,
    gate_hbm,
    up_hbm,
    updated_out,
    hidden_out,
    cache_out,
    lengths,
    routing,
    cache,
    queries,
    fresh,
    residual,
    gain,
    router,
    gate_w,
    up_w,
    residual_rows,
    stream,
    stream_rows,
    raw,
    scaled,
    normed,
    columns,
    tokens,
    routes,
    gate_all,
    up_all,
    partial,
    arrived,
    load_sem,
    local_sem,
    stream_send,
    stream_recv,
    raw_send,
    raw_recv,
    cache_send,
    cache_recv,
    route_send,
    route_recv,
    column_send,
    column_recv,
    sum_send,
    sum_recv,
):
    groups, tensors, span = dims
    mine = lax.axis_index("group")
    rank = lax.axis_index("tensor")
    pairs, slots, width = cache.shape
    head = width // 2
    seqs, cols = updated_out.shape
    parts = tensors // seqs
    seq = rank // parts
    part = lax.rem(rank, parts)
    heads = cols // parts // head
    share = heads // pairs
    blocks = cols // LANES
    own_blocks = blocks // groups
    pieces = groups // parts
    experts = gate_w.shape[0]
    hidden = gate_w.shape[2]
    home = mine // pieces
    at_home = home == part

    def tensor_peer(i):
        return lax.rem(rank + i, tensors)

    def group_peer(i):
        return lax.rem(mine + i, groups)

    def seq_peer(i):
        return lax.rem(seq + i, seqs)

    def part_peer(i):
        return lax.rem(part + i, parts)

    def remote(source, target, send, recv, **to):
        return pltpu.make_async_remote_copy(
            src_ref=source,
            dst_ref=target,
            send_sem=send,
            recv_sem=recv,
            device_id=to,
            device_id_type=MESH,
        )

    def cache_copy(to):
        return remote(
            cache.at[:, pl.ds(pl.multiple_of(to * span, span), span), :],
            cache_out.at[pl.ds(rank * pairs, pairs)],
            cache_send,
            cache_recv,
            tensor=to,
        )

    def stream_copy(to):
        return remote(
            stream.at[seq], stream.at[seq], stream_send, stream_recv, tensor=to * parts + part
        )

    def raw_copy(to):
        return remote(raw.at[part], raw.at[part], raw_send, raw_recv, tensor=seq * parts + to)

    def route_copy(to):
        return remote(routes.at[mine], routes.at[mine], route_send, route_recv, group=to)

    def column_copy(piece, to):
        return remote(
            scaled.at[pl.ds(piece * own_blocks, own_blocks)],
            columns.at[mine],
            column_send,
            column_recv,
            group=part * pieces + piece,
            tensor=seq * parts + to,
        )

    def sum_copy(to):
        return remote(partial.at[to], arrived.at[mine], sum_send, sum_recv, group=to)

    def signal(**to):
        pl.semaphore_signal(barrier, inc=1, device_id=to, device_id_type=MESH)

    def each(count, step):
        def go(i, carry):
            step(i)
            return carry

        lax.fori_loop(1, count, go, 0)

    loads = [
        pltpu.make_async_copy(source, target, load_sem.at[k])
        for k, (source, target) in enumerate(
            (
                (cache_hbm, cache),
                (lengths_hbm, lengths),
                (queries_hbm.at[seq], queries),
                (fresh_hbm.at[seq], fresh),
                (residual_hbm, residual),
                (routing_hbm, routing),
                (gain_hbm, gain),
                (router_hbm, router),
                (gate_hbm, gate_w),
                (up_hbm, up_w),
            )
        )
    ]
    for load in loads:
        load.start()

    barrier = pltpu.get_barrier_semaphore()
    for i in range(1, tensors):
        signal(tensor=tensor_peer(i))
    for i in range(1, groups):
        signal(group=group_peer(i))

    @pl.when(jnp.logical_not(at_home))
    def _():
        for i in range(groups):
            signal(group=i, tensor=seq * parts + home)

    @pl.when(at_home)
    def _():
        each(groups, lambda i: signal(group=group_peer(i)))

    for load in loads[:6]:
        load.wait()

    length = lengths[seq]
    fresh_rows = fresh[...].astype(jnp.float32)
    row_id = lax.broadcasted_iota(jnp.int32, fresh_rows.shape, 0)
    chunk = 128
    for p in range(pairs):
        own_row = jnp.sum(
            jnp.where(row_id == part * pairs + p, fresh_rows, 0.0), axis=0, keepdims=True
        )

        def place(c, carry, p=p, own_row=own_row):
            at = pl.ds(pl.multiple_of(c * chunk, chunk), chunk)
            slot_id = lax.broadcasted_iota(jnp.int32, (chunk, width), 0) + c * chunk
            cache[p, at, :] = jnp.where(
                slot_id == length, own_row, cache[p, at, :].astype(jnp.float32)
            ).astype(jnp.bfloat16)
            return carry

        lax.fori_loop(0, slots // chunk, place, 0)

    pick = (
        lax.broadcasted_iota(jnp.int32, (ROWS, queries.shape[0]), 1)
        == lax.broadcasted_iota(jnp.int32, (ROWS, queries.shape[0]), 0) + part * heads
    )
    own_queries = jnp.dot(
        pick.astype(jnp.float32).astype(jnp.bfloat16),
        queries[...],
        preferred_element_type=jnp.float32,
    ).astype(jnp.bfloat16)
    visible = lax.broadcasted_iota(jnp.int32, (ROWS, slots), 1) <= length
    out_row = lax.broadcasted_iota(jnp.int32, (ROWS, head), 0)
    attention = None
    for p in range(pairs):
        scores = lax.dot_general(
            own_queries, cache[p, :, :head], NT, preferred_element_type=jnp.float32
        ) * (1.0 / math.sqrt(head))
        scores = jnp.where(visible, scores, -1e30)
        peak = jnp.max(scores, axis=1, keepdims=True)
        weights = jnp.where(visible, jnp.exp(scores - peak), 0.0)
        denominator = jnp.sum(weights, axis=1, keepdims=True)
        weighted = jnp.dot(
            weights.astype(jnp.bfloat16), cache[p, :, head:], preferred_element_type=jnp.float32
        )
        result = weighted / denominator
        attention = result if p == 0 else jnp.where(out_row < p * share, attention, result)

    residual_rows[...] = jnp.zeros_like(residual_rows)
    for c in range(heads):
        at = pl.ds(pl.multiple_of(part * heads * LANES + c * LANES, LANES), LANES)
        residual_rows[c * seqs : (c + 1) * seqs, :] = residual[:, at].astype(jnp.float32)
    own_residual = residual_rows[pl.ds(seq, ROWS, stride=seqs), :]
    stream[seq] = (own_residual + attention).astype(jnp.bfloat16)

    sublane = lax.broadcasted_iota(jnp.int32, (seqs, LANES), 0)
    for k in range(routing.shape[0]):
        value = jnp.zeros((seqs, LANES), jnp.int32)
        for s in range(seqs):
            value = jnp.where(sublane == s, routing[k, s], value)
        routes[mine, k] = value

    pl.semaphore_wait(barrier, tensors + groups - 2 + groups - jnp.where(at_home, 1, 0))
    each(seqs, lambda i: stream_copy(seq_peer(i)).start())
    each(groups, lambda i: route_copy(group_peer(i)).start())
    keep = pltpu.make_async_copy(
        cache.at[:, pl.ds(pl.multiple_of(rank * span, span), span), :],
        cache_out.at[pl.ds(rank * pairs, pairs)],
        local_sem,
    )
    keep.start()
    each(tensors, lambda i: cache_copy(tensor_peer(i)).start())
    for load in loads[6:]:
        load.wait()
    others = stream.at[pl.ds(0, seqs - 1)]
    remote(others, others, stream_send, stream_recv, tensor=rank).wait_recv()

    for k in range(seqs):
        stream_rows[k * ROWS : (k + 1) * ROWS, :] = stream[k].astype(jnp.float32)
    for c in range(heads):
        tile = stream_rows[pl.ds(c, seqs, stride=ROWS), :]
        raw[part, c] = tile.astype(jnp.bfloat16)
        scaled[c] = (tile * gain[pl.ds(part * heads + c, 1), :]).astype(jnp.bfloat16)
    for piece in range(pieces):
        for i in range(1, parts):
            column_copy(piece, part_peer(i)).start()

        @pl.when(part * pieces + piece != mine)
        def _():
            column_copy(piece, part).start()

    own_columns = pltpu.make_async_copy(
        scaled.at[pl.ds(lax.rem(mine, pieces) * own_blocks, own_blocks)],
        columns.at[mine],
        column_recv,
    )

    @pl.when(at_home)
    def _():
        own_columns.start()

    each(parts, lambda i: raw_copy(part_peer(i)).start())

    other_routes = routes.at[pl.ds(0, groups - 1)]
    remote(other_routes, other_routes, route_send, route_recv, group=mine).wait_recv()
    remote(columns, columns, column_send, column_recv, group=mine).wait_recv()
    for c in range(own_blocks):
        tokens[:, c * LANES : (c + 1) * LANES] = (
            columns[:, c].astype(jnp.float32).reshape(groups * seqs, LANES).astype(jnp.bfloat16)
        )
    for e in range(experts):
        gate_all[e] = jnp.dot(tokens[...], gate_w[e], preferred_element_type=jnp.float32)
        up_all[e] = jnp.dot(tokens[...], up_w[e], preferred_element_type=jnp.float32)

    def choose(to):
        at = pl.ds(pl.multiple_of(to * seqs, seqs), seqs)
        for k in range(2):
            route = routes[to, k]
            route = jnp.concatenate([route] * (hidden // LANES), axis=1)
            for q, source in enumerate((gate_all, up_all)):
                value = source[0, at, :]
                for e in range(1, experts):
                    value = jnp.where(route == e, source[e, at, :], value)
                partial[to, 2 * k + q] = value.astype(jnp.bfloat16)

    def choose_and_send(i):
        choose(group_peer(i))

        @pl.when(i > 1)
        def _():
            sum_copy(group_peer(i - 1)).start()

    each(groups, choose_and_send)
    choose(mine)
    sum_copy(group_peer(groups - 1)).start()
    arrived[mine] = partial[mine]

    other_parts = raw.at[pl.ds(0, parts - 1)]
    remote(other_parts, other_parts, raw_send, raw_recv, group=mine).wait_recv()
    total = jnp.zeros((seqs, LANES), jnp.float32)
    for c in range(blocks):
        value = raw[c // heads, c % heads]
        updated_out[:, c * LANES : (c + 1) * LANES] = value
        value = value.astype(jnp.float32)
        total = total + value * value
    scale = lax.rsqrt(jnp.sum(total, axis=1, keepdims=True) / cols + 1e-05)
    for c in range(blocks):
        value = raw[c // heads, c % heads].astype(jnp.float32)
        normed[:, c * LANES : (c + 1) * LANES] = (value * scale * gain[c : c + 1, :]).astype(
            jnp.bfloat16
        )
    logits = lax.dot_general(normed[...], router[...], NT, preferred_element_type=jnp.float32)
    expert_id = lax.broadcasted_iota(jnp.int32, (seqs, experts), 1)
    chosen = [
        jnp.sum(
            jnp.where(routes[mine, k][:, :1] == expert_id, logits, 0.0), axis=1, keepdims=True
        )
        for k in range(2)
    ]
    gate_weights = [
        1.0 / (1.0 + jnp.exp(chosen[1] - chosen[0])),
        1.0 / (1.0 + jnp.exp(chosen[0] - chosen[1])),
    ]

    other_sums = arrived.at[pl.ds(0, groups - 1)]
    remote(other_sums, other_sums, sum_send, sum_recv, group=mine).wait_recv()
    units = []
    for k in range(2):
        sums = []
        for q in range(2):
            value = arrived[0, 2 * k + q].astype(jnp.float32)
            for s in range(1, groups):
                value = value + arrived[s, 2 * k + q].astype(jnp.float32)
            sums.append(value * scale)
        silu = sums[0] / (1.0 + jnp.exp(-sums[0]))
        units.append(gate_weights[k] * silu * sums[1])
    for s in range(seqs):
        hidden_out[s] = jnp.concatenate([unit[s : s + 1] for unit in units], axis=0).astype(
            jnp.bfloat16
        )

    remote(others, others, stream_send, stream_recv, tensor=rank).wait_send()
    remote(other_routes, other_routes, route_send, route_recv, group=mine).wait_send()
    remote(other_parts, other_parts, raw_send, raw_recv, group=mine).wait_send()
    remote(other_sums, other_sums, sum_send, sum_recv, group=mine).wait_send()
    most = columns.at[pl.ds(0, groups - 1)]
    remote(most, most, column_send, column_recv, group=mine).wait_send()

    @pl.when(jnp.logical_not(at_home))
    def _():
        one = columns.at[0]
        remote(one, one, column_send, column_recv, group=mine).wait_send()

    most_cache = cache_out.at[pl.ds(0, (tensors - 1) * pairs)]
    remote(most_cache, most_cache, cache_send, cache_recv, tensor=rank).wait_send()
    keep.wait()
    remote(most_cache, most_cache, cache_send, cache_recv, tensor=rank).wait_recv()


def write_out(updated, hidden_units, cache, updated_hbm, hidden_hbm, cache_hbm, sems):
    copies = [
        pltpu.make_async_copy(source, target, sems.at[k])
        for k, (source, target) in enumerate(
            ((cache, cache_hbm), (updated, updated_hbm), (hidden_units, hidden_hbm))
        )
    ]
    for copy in copies:
        copy.start()
    for copy in copies:
        copy.wait()


def body(
    groups,
    tensors,
    key_value_cache,
    queries,
    fresh_key_value,
    lengths,
    residual,
    norm_gain,
    router_weight,
    routing,
    expert_gate,
    expert_up,
):
    pairs, slots, width = key_value_cache.shape
    seqs, q_heads, head = queries.shape
    kv_heads = fresh_key_value.shape[1]
    cols = residual.shape[1]
    experts, own_cols, hidden = expert_gate.shape
    span = slots // tensors
    parts = tensors // seqs
    heads = cols // parts // head
    bf16, f32, i32 = jnp.bfloat16, jnp.float32, jnp.int32
    dma = pltpu.SemaphoreType.DMA
    hbm = pl.BlockSpec(memory_space=pltpu.HBM)
    vmem = pl.BlockSpec(memory_space=pltpu.VMEM)
    updated, hidden_units, new_cache = pl.pallas_call(
        functools.partial(kernel, (groups, tensors, span)),
        out_shape=(
            pltpu.VMEM((seqs, cols), bf16),
            pltpu.VMEM((seqs, 2, hidden), bf16),
            pltpu.VMEM((seqs * kv_heads, span, width), bf16),
        ),
        in_specs=[hbm] * 10,
        out_specs=(vmem, vmem, vmem),
        scratch_shapes=[
            pltpu.SMEM((seqs,), i32),
            pltpu.SMEM((2, seqs), i32),
            pltpu.VMEM((pairs, slots, width), bf16),
            pltpu.VMEM((q_heads, head), bf16),
            pltpu.VMEM((kv_heads, width), bf16),
            pltpu.VMEM((seqs, cols), bf16),
            pltpu.VMEM((cols // LANES, LANES), f32),
            pltpu.VMEM((experts, cols), bf16),
            pltpu.VMEM(expert_gate.shape, bf16),
            pltpu.VMEM(expert_up.shape, bf16),
            pltpu.VMEM((ROWS * seqs, LANES), f32),
            pltpu.VMEM((seqs, ROWS, LANES), bf16),
            pltpu.VMEM((seqs * ROWS, LANES), f32),
            pltpu.VMEM((parts, heads, seqs, LANES), bf16),
            pltpu.VMEM((heads, seqs, LANES), bf16),
            pltpu.VMEM((seqs, cols), bf16),
            pltpu.VMEM((groups, own_cols // LANES, seqs, LANES), bf16),
            pltpu.VMEM((groups * seqs, own_cols), bf16),
            pltpu.VMEM((groups, 2, seqs, LANES), i32),
            pltpu.VMEM((experts, groups * seqs, hidden), f32),
            pltpu.VMEM((experts, groups * seqs, hidden), f32),
            pltpu.VMEM((groups, 4, seqs, hidden), bf16),
            pltpu.VMEM((groups, 4, seqs, hidden), bf16),
            dma((10,)),
        ]
        + [dma(())] * 13,
        compiler_params=pltpu.CompilerParams(
            collective_id=0, has_side_effects=True
        ),
    )(
        lengths,
        routing.T,
        key_value_cache,
        queries,
        fresh_key_value,
        residual,
        norm_gain.reshape(cols // LANES, LANES),
        router_weight.T,
        expert_gate,
        expert_up,
    )
    updated, hidden_units, new_cache = pl.pallas_call(
        write_out,
        out_shape=(
            jax.ShapeDtypeStruct(updated.shape, bf16),
            jax.ShapeDtypeStruct(hidden_units.shape, bf16),
            jax.ShapeDtypeStruct(new_cache.shape, bf16),
        ),
        in_specs=[vmem] * 3,
        out_specs=(hbm,) * 3,
        scratch_shapes=[dma((3,))],
        compiler_params=pltpu.CompilerParams(vmem_limit_bytes=4 << 20),
    )(updated, hidden_units, new_cache)
    return (
        updated,
        hidden_units,
        new_cache.reshape(seqs, kv_heads, span, width),
    )


def solution(mesh):
    in_specs = (
        P(("group", "tensor"), None, None),
        P("group", None, None),
        P("group", None, None),
        P("group"),
        P("group", None),
        P(),
        P(),
        P("group", None),
        P(None, "group", "tensor"),
        P(None, "group", "tensor"),
    )
    out_specs = (P("group", None), P("group", None, "tensor"), P("group", None, "tensor", None))
    return jax.shard_map(
        functools.partial(body, mesh.shape["group"], mesh.shape["tensor"]),
        mesh=mesh,
        in_specs=in_specs,
        out_specs=out_specs,
        check_vma=False,
    )
```

```python
import functools
import math

import jax
import jax.numpy as jnp
from jax import lax
from jax.experimental import pallas as pl
from jax.experimental.pallas import tpu as pltpu
from jax.sharding import PartitionSpec as P

MESH = pl.DeviceIdType.MESH
LANES = 128
ROWS = 16
NT = (((1,), (1,)), ((), ()))


def FIRST(down, along):
    return along == 0


def kernel(
    dims,
    lengths_hbm,
    routing_hbm,
    cache_hbm,
    queries_hbm,
    fresh_hbm,
    residual_hbm,
    gain_hbm,
    router_hbm,
    gate_hbm,
    up_hbm,
    updated_out,
    hidden_out,
    cache_out,
    lengths,
    routing,
    cache,
    queries,
    fresh,
    residual,
    gain,
    router,
    gate_w,
    up_w,
    residual_rows,
    stream,
    stream_rows,
    raw,
    scaled,
    normed,
    columns,
    tokens,
    routes,
    gate_all,
    up_all,
    pair_out,
    pair_in,
    pair_own,
    partial,
    arrived,
    load_sem,
    local_sem,
    stream_send,
    stream_recv,
    raw_send,
    raw_recv,
    cache_send,
    cache_recv,
    route_send,
    route_recv,
    column_send,
    column_recv,
    pair_send,
    pair_recv,
    sum_send,
    sum_recv,
):
    groups, tensors, span = dims
    mine = lax.axis_index("group")
    rank = lax.axis_index("tensor")
    pairs, slots, width = cache.shape
    head = width // 2
    seqs, cols = updated_out.shape
    parts = tensors // seqs
    seq = rank // parts
    part = lax.rem(rank, parts)
    heads = cols // parts // head
    share = heads // pairs
    blocks = cols // LANES
    own_blocks = blocks // groups
    pieces = groups // parts
    experts = gate_w.shape[0]
    hidden = gate_w.shape[2]
    chips = groups // 2
    chip = mine // 2
    core = lax.rem(mine, 2)
    lower = mine < chips

    def group_peer(i):
        return lax.rem(mine + i, groups)

    def seq_peer(i):
        return lax.rem(seq + i, seqs)

    def part_peer(i):
        return lax.rem(part + i, parts)

    def chip_peer(i):
        return lax.rem(chip + i, chips)

    def tensor_peer(down, along):
        return lax.rem(seq + down, seqs) * parts + lax.rem(part + along, parts)

    offsets = sorted(
        ((down, along) for down in range(seqs) for along in range(parts) if down or along),
        key=lambda o: -min(o[0], seqs - o[0]) - min(o[1], parts - o[1]),
    )

    def remote(source, target, send, recv, **to):
        return pltpu.make_async_remote_copy(
            src_ref=source,
            dst_ref=target,
            send_sem=send,
            recv_sem=recv,
            device_id=to,
            device_id_type=MESH,
        )

    def cache_copy(to):
        return remote(
            cache.at[:, pl.ds(pl.multiple_of(to * span, span), span), :],
            cache_out.at[pl.ds(rank * pairs, pairs)],
            cache_send,
            cache_recv,
            tensor=to,
        )

    def stream_copy(to):
        return remote(
            stream.at[seq], stream.at[seq], stream_send, stream_recv, tensor=to * parts + part
        )

    def raw_copy(to):
        return remote(raw.at[part], raw.at[part], raw_send, raw_recv, tensor=seq * parts + to)

    def route_copy(to):
        return remote(routes.at[mine], routes.at[mine], route_send, route_recv, group=to)

    def column_copy(to):
        return remote(
            scaled.at[pl.ds(to * own_blocks, own_blocks)],
            columns.at[mine],
            column_send,
            column_recv,
            group=to,
        )

    def sum_copy(to):
        return remote(
            partial.at[to], arrived.at[chip], sum_send, sum_recv, group=2 * to + core
        )

    def signal(**to):
        pl.semaphore_signal(barrier, inc=1, device_id=to, device_id_type=MESH)

    def each(count, step):
        def go(i, carry):
            step(i)
            return carry

        lax.fori_loop(1, count, go, 0)

    loads = [
        pltpu.make_async_copy(source, target, load_sem.at[k])
        for k, (source, target) in enumerate(
            (
                (cache_hbm, cache),
                (lengths_hbm, lengths),
                (queries_hbm.at[seq], queries),
                (fresh_hbm.at[seq], fresh),
                (residual_hbm, residual),
                (routing_hbm, routing),
                (gain_hbm, gain),
                (router_hbm, router),
                (gate_hbm, gate_w),
                (up_hbm, up_w),
            )
        )
    ]
    for load in loads:
        load.start()

    barrier = pltpu.get_barrier_semaphore()
    for offset in offsets:
        signal(tensor=tensor_peer(*offset))

    for load in loads[:6]:
        load.wait()

    length = lengths[seq]
    fresh_rows = fresh[...].astype(jnp.float32)
    row_id = lax.broadcasted_iota(jnp.int32, fresh_rows.shape, 0)
    chunk = 128
    for p in range(pairs):
        own_row = jnp.sum(
            jnp.where(row_id == part * pairs + p, fresh_rows, 0.0), axis=0, keepdims=True
        )

        def place(c, carry, p=p, own_row=own_row):
            at = pl.ds(pl.multiple_of(c * chunk, chunk), chunk)
            slot_id = lax.broadcasted_iota(jnp.int32, (chunk, width), 0) + c * chunk
            cache[p, at, :] = jnp.where(
                slot_id == length, own_row, cache[p, at, :].astype(jnp.float32)
            ).astype(jnp.bfloat16)
            return carry

        lax.fori_loop(0, slots // chunk, place, 0)

    pick = (
        lax.broadcasted_iota(jnp.int32, (ROWS, queries.shape[0]), 1)
        == lax.broadcasted_iota(jnp.int32, (ROWS, queries.shape[0]), 0) + part * heads
    )
    own_queries = jnp.dot(
        pick.astype(jnp.float32).astype(jnp.bfloat16),
        queries[...],
        preferred_element_type=jnp.float32,
    ).astype(jnp.bfloat16)
    visible = lax.broadcasted_iota(jnp.int32, (ROWS, slots), 1) <= length
    out_row = lax.broadcasted_iota(jnp.int32, (ROWS, head), 0)
    attention = None
    for p in range(pairs):
        scores = lax.dot_general(
            own_queries, cache[p, :, :head], NT, preferred_element_type=jnp.float32
        ) * (1.0 / math.sqrt(head))
        scores = jnp.where(visible, scores, -1e30)
        peak = jnp.max(scores, axis=1, keepdims=True)
        weights = jnp.where(visible, jnp.exp(scores - peak), 0.0)
        denominator = jnp.sum(weights, axis=1, keepdims=True)
        weighted = jnp.dot(
            weights.astype(jnp.bfloat16), cache[p, :, head:], preferred_element_type=jnp.float32
        )
        result = weighted / denominator
        attention = result if p == 0 else jnp.where(out_row < p * share, attention, result)

    residual_rows[...] = jnp.zeros_like(residual_rows)
    for c in range(heads):
        at = pl.ds(pl.multiple_of(part * heads * LANES + c * LANES, LANES), LANES)
        residual_rows[c * seqs : (c + 1) * seqs, :] = residual[:, at].astype(jnp.float32)
    own_residual = residual_rows[pl.ds(seq, ROWS, stride=seqs), :]
    stream[seq] = (own_residual + attention).astype(jnp.bfloat16)

    sublane = lax.broadcasted_iota(jnp.int32, (seqs, LANES), 0)
    for k in range(routing.shape[0]):
        value = jnp.zeros((seqs, LANES), jnp.int32)
        for s in range(seqs):
            value = jnp.where(sublane == s, routing[k, s], value)
        routes[mine, k] = value

    pl.semaphore_wait(barrier, tensors - 1 + jnp.where(lower, 0, chips))
    each(seqs, lambda i: stream_copy(seq_peer(i)).start())

    @pl.when(lower)
    def _():
        for i in range(chips, groups):
            signal(group=i)

    @pl.when(jnp.logical_not(lower))
    def _():
        for i in range(chips):
            signal(group=i)

    keep = pltpu.make_async_copy(
        cache.at[:, pl.ds(pl.multiple_of(rank * span, span), span), :],
        cache_out.at[pl.ds(rank * pairs, pairs)],
        local_sem,
    )
    keep.start()
    for offset in offsets:
        if FIRST(*offset):
            cache_copy(tensor_peer(*offset)).start()
    for load in loads[6:]:
        load.wait()
    others = stream.at[pl.ds(0, seqs - 1)]
    remote(others, others, stream_send, stream_recv, tensor=rank).wait_recv()

    def scale_part(at):
        for c in range(heads):
            tile = raw[at, c].astype(jnp.float32)
            scaled[at * heads + c] = (tile * gain[pl.ds(at * heads + c, 1), :]).astype(
                jnp.bfloat16
            )

    for k in range(seqs):
        stream_rows[k * ROWS : (k + 1) * ROWS, :] = stream[k].astype(jnp.float32)
    for c in range(heads):
        raw[part, c] = stream_rows[pl.ds(c, seqs, stride=ROWS), :].astype(jnp.bfloat16)
    each(parts, lambda i: raw_copy(part_peer(i)).start())
    for offset in offsets:
        if not FIRST(*offset):
            cache_copy(tensor_peer(*offset)).start()
    scale_part(part)

    @pl.when(lower)
    def _():
        pl.semaphore_wait(barrier, chips)
        signal(group=groups - 1 - mine)

    @pl.when(jnp.logical_not(lower))
    def _():
        pl.semaphore_wait(barrier, 1)

    each(groups, lambda i: route_copy(group_peer(i)).start())
    def send_part(at):
        for piece in range(pieces):
            to = at * pieces + piece

            @pl.when(to != mine)
            def _():
                column_copy(to).start()

    send_part(part)
    other_parts = raw.at[pl.ds(0, parts - 1)]
    remote(other_parts, other_parts, raw_send, raw_recv, group=mine).wait_recv()
    for i in range(1, parts):
        scale_part(part_peer(i))
    for i in range(1, parts):
        send_part(part_peer(i))
    columns[mine] = scaled[pl.ds(mine * own_blocks, own_blocks)]

    other_routes = routes.at[pl.ds(0, groups - 1)]
    remote(other_routes, other_routes, route_send, route_recv, group=mine).wait_recv()
    most = columns.at[pl.ds(0, groups - 1)]
    remote(most, most, column_send, column_recv, group=mine).wait_recv()
    for c in range(own_blocks):
        tokens[:, c * LANES : (c + 1) * LANES] = (
            columns[:, c].astype(jnp.float32).reshape(groups * seqs, LANES).astype(jnp.bfloat16)
        )
    for e in range(experts):
        gate_all[e] = jnp.dot(tokens[...], gate_w[e], preferred_element_type=jnp.float32)
        up_all[e] = jnp.dot(tokens[...], up_w[e], preferred_element_type=jnp.float32)

    def choose(to, target, at):
        rows = pl.ds(pl.multiple_of(to * seqs, seqs), seqs)
        for k in range(2):
            route = routes[to, k]
            route = jnp.concatenate([route] * (hidden // LANES), axis=1)
            for q, source in enumerate((gate_all, up_all)):
                value = source[0, rows, :]
                for e in range(1, experts):
                    value = jnp.where(route == e, source[e, rows, :], value)
                target[at, 2 * k + q] = value.astype(target.dtype)

    def for_pair(i, carry):
        choose(2 * i + 1 - core, pair_out, i)
        return carry

    def for_own(i, carry):
        choose(2 * i + core, pair_own, i)
        return carry

    lax.fori_loop(0, chips, for_pair, 0)
    pair = remote(pair_out, pair_in, pair_send, pair_recv, group=2 * chip + 1 - core)
    pair.start()
    lax.fori_loop(0, chips, for_own, 0)
    pair.wait_recv()

    def add_pair(to):
        partial[to] = (pair_own[to] + pair_in[to].astype(jnp.float32)).astype(jnp.bfloat16)

    def add_and_send(i):
        add_pair(chip_peer(i))

        @pl.when(i > 1)
        def _():
            sum_copy(chip_peer(i - 1)).start()

    each(chips, add_and_send)
    add_pair(chip)
    sum_copy(chip_peer(chips - 1)).start()
    arrived[chip] = partial[chip]

    total = jnp.zeros((seqs, LANES), jnp.float32)
    for c in range(blocks):
        value = raw[c // heads, c % heads]
        updated_out[:, c * LANES : (c + 1) * LANES] = value
        value = value.astype(jnp.float32)
        total = total + value * value
    scale = lax.rsqrt(jnp.sum(total, axis=1, keepdims=True) / cols + 1e-05)
    for c in range(blocks):
        value = raw[c // heads, c % heads].astype(jnp.float32)
        normed[:, c * LANES : (c + 1) * LANES] = (value * scale * gain[c : c + 1, :]).astype(
            jnp.bfloat16
        )
    logits = lax.dot_general(normed[...], router[...], NT, preferred_element_type=jnp.float32)
    expert_id = lax.broadcasted_iota(jnp.int32, (seqs, experts), 1)
    chosen = [
        jnp.sum(
            jnp.where(routes[mine, k][:, :1] == expert_id, logits, 0.0), axis=1, keepdims=True
        )
        for k in range(2)
    ]
    gate_weights = [
        1.0 / (1.0 + jnp.exp(chosen[1] - chosen[0])),
        1.0 / (1.0 + jnp.exp(chosen[0] - chosen[1])),
    ]

    other_sums = arrived.at[pl.ds(0, chips - 1)]
    remote(other_sums, other_sums, sum_send, sum_recv, group=mine).wait_recv()
    units = []
    for k in range(2):
        sums = []
        for q in range(2):
            value = arrived[0, 2 * k + q].astype(jnp.float32)
            for s in range(1, chips):
                value = value + arrived[s, 2 * k + q].astype(jnp.float32)
            sums.append(value * scale)
        silu = sums[0] / (1.0 + jnp.exp(-sums[0]))
        units.append(gate_weights[k] * silu * sums[1])
    for s in range(seqs):
        hidden_out[s] = jnp.concatenate([unit[s : s + 1] for unit in units], axis=0).astype(
            jnp.bfloat16
        )

    remote(others, others, stream_send, stream_recv, tensor=rank).wait_send()
    remote(other_routes, other_routes, route_send, route_recv, group=mine).wait_send()
    remote(other_parts, other_parts, raw_send, raw_recv, group=mine).wait_send()
    pair.wait_send()
    remote(other_sums, other_sums, sum_send, sum_recv, group=mine).wait_send()
    remote(most, most, column_send, column_recv, group=mine).wait_send()

    most_cache = cache_out.at[pl.ds(0, (tensors - 1) * pairs)]
    remote(most_cache, most_cache, cache_send, cache_recv, tensor=rank).wait_send()
    keep.wait()
    remote(most_cache, most_cache, cache_send, cache_recv, tensor=rank).wait_recv()


def write_out(updated, hidden_units, cache, updated_hbm, hidden_hbm, cache_hbm, sems):
    copies = [
        pltpu.make_async_copy(source, target, sems.at[k])
        for k, (source, target) in enumerate(
            ((cache, cache_hbm), (updated, updated_hbm), (hidden_units, hidden_hbm))
        )
    ]
    for copy in copies:
        copy.start()
    for copy in copies:
        copy.wait()


def body(
    groups,
    tensors,
    key_value_cache,
    queries,
    fresh_key_value,
    lengths,
    residual,
    norm_gain,
    router_weight,
    routing,
    expert_gate,
    expert_up,
):
    pairs, slots, width = key_value_cache.shape
    seqs, q_heads, head = queries.shape
    kv_heads = fresh_key_value.shape[1]
    cols = residual.shape[1]
    experts, own_cols, hidden = expert_gate.shape
    span = slots // tensors
    parts = tensors // seqs
    heads = cols // parts // head
    bf16, f32, i32 = jnp.bfloat16, jnp.float32, jnp.int32
    dma = pltpu.SemaphoreType.DMA
    hbm = pl.BlockSpec(memory_space=pltpu.HBM)
    vmem = pl.BlockSpec(memory_space=pltpu.VMEM)
    updated, hidden_units, new_cache = pl.pallas_call(
        functools.partial(kernel, (groups, tensors, span)),
        out_shape=(
            pltpu.VMEM((seqs, cols), bf16),
            pltpu.VMEM((seqs, 2, hidden), bf16),
            pltpu.VMEM((seqs * kv_heads, span, width), bf16),
        ),
        in_specs=[hbm] * 10,
        out_specs=(vmem, vmem, vmem),
        scratch_shapes=[
            pltpu.SMEM((seqs,), i32),
            pltpu.SMEM((2, seqs), i32),
            pltpu.VMEM((pairs, slots, width), bf16),
            pltpu.VMEM((q_heads, head), bf16),
            pltpu.VMEM((kv_heads, width), bf16),
            pltpu.VMEM((seqs, cols), bf16),
            pltpu.VMEM((cols // LANES, LANES), f32),
            pltpu.VMEM((experts, cols), bf16),
            pltpu.VMEM(expert_gate.shape, bf16),
            pltpu.VMEM(expert_up.shape, bf16),
            pltpu.VMEM((ROWS * seqs, LANES), f32),
            pltpu.VMEM((seqs, ROWS, LANES), bf16),
            pltpu.VMEM((seqs * ROWS, LANES), f32),
            pltpu.VMEM((parts, heads, seqs, LANES), bf16),
            pltpu.VMEM((parts * heads, seqs, LANES), bf16),
            pltpu.VMEM((seqs, cols), bf16),
            pltpu.VMEM((groups, own_cols // LANES, seqs, LANES), bf16),
            pltpu.VMEM((groups * seqs, own_cols), bf16),
            pltpu.VMEM((groups, 2, seqs, LANES), i32),
            pltpu.VMEM((experts, groups * seqs, hidden), f32),
            pltpu.VMEM((experts, groups * seqs, hidden), f32),
            pltpu.VMEM((groups // 2, 4, seqs, hidden), bf16),
            pltpu.VMEM((groups // 2, 4, seqs, hidden), bf16),
            pltpu.VMEM((groups // 2, 4, seqs, hidden), f32),
            pltpu.VMEM((groups // 2, 4, seqs, hidden), bf16),
            pltpu.VMEM((groups // 2, 4, seqs, hidden), bf16),
            dma((10,)),
        ]
        + [dma(())] * 15,
        compiler_params=pltpu.CompilerParams(
            collective_id=0, has_side_effects=True
        ),
    )(
        lengths,
        routing.T,
        key_value_cache,
        queries,
        fresh_key_value,
        residual,
        norm_gain.reshape(cols // LANES, LANES),
        router_weight.T,
        expert_gate,
        expert_up,
    )
    updated, hidden_units, new_cache = pl.pallas_call(
        write_out,
        out_shape=(
            jax.ShapeDtypeStruct(updated.shape, bf16),
            jax.ShapeDtypeStruct(hidden_units.shape, bf16),
            jax.ShapeDtypeStruct(new_cache.shape, bf16),
        ),
        in_specs=[vmem] * 3,
        out_specs=(hbm,) * 3,
        scratch_shapes=[dma((3,))],
        compiler_params=pltpu.CompilerParams(vmem_limit_bytes=4 << 20),
    )(updated, hidden_units, new_cache)
    return (
        updated,
        hidden_units,
        new_cache.reshape(seqs, kv_heads, span, width),
    )


def solution(mesh):
    in_specs = (
        P(("group", "tensor"), None, None),
        P("group", None, None),
        P("group", None, None),
        P("group"),
        P("group", None),
        P(),
        P(),
        P("group", None),
        P(None, "group", "tensor"),
        P(None, "group", "tensor"),
    )
    out_specs = (P("group", None), P("group", None, "tensor"), P("group", None, "tensor", None))
    return jax.shard_map(
        functools.partial(body, mesh.shape["group"], mesh.shape["tensor"]),
        mesh=mesh,
        in_specs=in_specs,
        out_specs=out_specs,
        check_vma=False,
    )
```

```python
import functools
import math

import jax
import jax.numpy as jnp
from jax import lax
from jax.experimental import pallas as pl
from jax.experimental.pallas import tpu as pltpu
from jax.sharding import PartitionSpec as P

MESH = pl.DeviceIdType.MESH
LANES = 128
ROWS = 16
NT = (((1,), (1,)), ((), ()))


def FIRST(down, along):
    return along == 0


def kernel(
    dims,
    lengths_hbm,
    routing_hbm,
    cache_hbm,
    queries_hbm,
    fresh_hbm,
    residual_hbm,
    gain_hbm,
    router_hbm,
    gate_hbm,
    up_hbm,
    updated_out,
    hidden_out,
    cache_out,
    lengths,
    routing,
    cache,
    queries,
    fresh,
    residual,
    gain,
    router,
    gate_w,
    up_w,
    residual_rows,
    stream,
    stream_rows,
    raw,
    scaled,
    normed,
    columns,
    tokens,
    routes,
    gate_all,
    up_all,
    pair_out,
    pair_in,
    pair_own,
    partial,
    arrived,
    load_sem,
    local_sem,
    stream_send,
    stream_recv,
    raw_send,
    raw_recv,
    cache_send,
    cache_recv,
    column_send,
    column_recv,
    pair_send,
    pair_recv,
    sum_send,
    sum_recv,
):
    groups, tensors, span = dims
    mine = lax.axis_index("group")
    rank = lax.axis_index("tensor")
    pairs, slots, width = cache.shape
    head = width // 2
    seqs, cols = updated_out.shape
    parts = tensors // seqs
    seq = rank // parts
    part = lax.rem(rank, parts)
    heads = cols // parts // head
    share = heads // pairs
    blocks = cols // LANES
    own_blocks = blocks // groups
    pieces = groups // parts
    experts = gate_w.shape[0]
    hidden = gate_w.shape[2]
    chips = groups // 2
    chip = mine // 2
    core = lax.rem(mine, 2)
    lower = mine < chips
    batch = mine // chips
    half = chips // 2

    def group_peer(i):
        return lax.rem(mine + i, groups)

    def seq_peer(i):
        return lax.rem(seq + i, seqs)

    def part_peer(i):
        return lax.rem(part + i, parts)

    def chip_peer(i):
        return lax.rem(chip + i, chips)

    def tensor_peer(down, along):
        return lax.rem(seq + down, seqs) * parts + lax.rem(part + along, parts)

    offsets = sorted(
        ((down, along) for down in range(seqs) for along in range(parts) if down or along),
        key=lambda o: -min(o[0], seqs - o[0]) - min(o[1], parts - o[1]),
    )

    def remote(source, target, send, recv, **to):
        return pltpu.make_async_remote_copy(
            src_ref=source,
            dst_ref=target,
            send_sem=send,
            recv_sem=recv,
            device_id=to,
            device_id_type=MESH,
        )

    def cache_copy(to):
        return remote(
            cache.at[:, pl.ds(pl.multiple_of(to * span, span), span), :],
            cache_out.at[pl.ds(rank * pairs, pairs)],
            cache_send,
            cache_recv,
            tensor=to,
        )

    def stream_copy(to):
        return remote(
            stream.at[seq], stream.at[seq], stream_send, stream_recv, tensor=to * parts + part
        )

    def raw_copy(to):
        return remote(raw.at[part], raw.at[part], raw_send, raw_recv, tensor=seq * parts + to)

    def column_copy(to):
        return remote(
            scaled.at[to],
            columns.at[mine],
            column_send,
            column_recv.at[batch],
            group=to,
        )

    def sum_copy(to):
        return remote(
            partial.at[to], arrived.at[chip], sum_send, sum_recv, group=2 * to + core
        )

    def signal(**to):
        pl.semaphore_signal(barrier, inc=1, device_id=to, device_id_type=MESH)

    def each(count, step):
        def go(i, carry):
            step(i)
            return carry

        lax.fori_loop(1, count, go, 0)

    loads = [
        pltpu.make_async_copy(source, target, load_sem.at[k])
        for k, (source, target) in enumerate(
            (
                (cache_hbm, cache),
                (lengths_hbm, lengths),
                (queries_hbm.at[seq], queries),
                (fresh_hbm.at[seq], fresh),
                (residual_hbm, residual),
                (routing_hbm, routing),
                (gain_hbm, gain),
                (router_hbm, router),
                (gate_hbm, gate_w),
                (up_hbm, up_w),
            )
        )
    ]
    for load in loads:
        load.start()

    barrier = pltpu.get_barrier_semaphore()
    for offset in offsets:
        signal(tensor=tensor_peer(*offset))

    for load in loads[:6]:
        load.wait()

    length = lengths[seq]
    fresh_rows = fresh[...].astype(jnp.float32)
    row_id = lax.broadcasted_iota(jnp.int32, fresh_rows.shape, 0)
    chunk = 128
    for p in range(pairs):
        own_row = jnp.sum(
            jnp.where(row_id == part * pairs + p, fresh_rows, 0.0), axis=0, keepdims=True
        )

        def place(c, carry, p=p, own_row=own_row):
            at = pl.ds(pl.multiple_of(c * chunk, chunk), chunk)
            slot_id = lax.broadcasted_iota(jnp.int32, (chunk, width), 0) + c * chunk
            cache[p, at, :] = jnp.where(
                slot_id == length, own_row, cache[p, at, :].astype(jnp.float32)
            ).astype(jnp.bfloat16)
            return carry

        lax.fori_loop(0, slots // chunk, place, 0)

    pick = (
        lax.broadcasted_iota(jnp.int32, (ROWS, queries.shape[0]), 1)
        == lax.broadcasted_iota(jnp.int32, (ROWS, queries.shape[0]), 0) + part * heads
    )
    own_queries = jnp.dot(
        pick.astype(jnp.float32).astype(jnp.bfloat16),
        queries[...],
        preferred_element_type=jnp.float32,
    ).astype(jnp.bfloat16)
    visible = lax.broadcasted_iota(jnp.int32, (ROWS, slots), 1) <= length
    out_row = lax.broadcasted_iota(jnp.int32, (ROWS, head), 0)
    attention = None
    for p in range(pairs):
        scores = lax.dot_general(
            own_queries, cache[p, :, :head], NT, preferred_element_type=jnp.float32
        ) * (1.0 / math.sqrt(head))
        scores = jnp.where(visible, scores, -1e30)
        peak = jnp.max(scores, axis=1, keepdims=True)
        weights = jnp.where(visible, jnp.exp(scores - peak), 0.0)
        denominator = jnp.sum(weights, axis=1, keepdims=True)
        weighted = jnp.dot(
            weights.astype(jnp.bfloat16), cache[p, :, head:], preferred_element_type=jnp.float32
        )
        result = weighted / denominator
        attention = result if p == 0 else jnp.where(out_row < p * share, attention, result)

    residual_rows[...] = jnp.zeros_like(residual_rows)
    for c in range(heads):
        at = pl.ds(pl.multiple_of(part * heads * LANES + c * LANES, LANES), LANES)
        residual_rows[c * seqs : (c + 1) * seqs, :] = residual[:, at].astype(jnp.float32)
    own_residual = residual_rows[pl.ds(seq, ROWS, stride=seqs), :]
    stream[seq] = (own_residual + attention).astype(jnp.bfloat16)

    sublane = lax.broadcasted_iota(jnp.int32, (seqs, LANES), 0)
    for k in range(routing.shape[0]):
        value = jnp.zeros((seqs, LANES), jnp.int32)
        for s in range(seqs):
            value = jnp.where(sublane == s, routing[k, s], value)
        routes[k] = value
    lane = lax.broadcasted_iota(jnp.int32, (seqs, LANES), 1)
    both = jnp.where(lane < LANES // 2, routes[0], routes[1])
    for to in range(groups):
        scaled[to, own_blocks] = both.astype(jnp.float32).astype(jnp.bfloat16)

    pl.semaphore_wait(barrier, tensors - 1 + jnp.where(lower, 0, chips))
    for i in sorted(range(1, seqs), key=lambda i: -min(i, seqs - i)):
        stream_copy(seq_peer(i)).start()

    @pl.when(lower)
    def _():
        for i in range(chips, groups):
            signal(group=i)

    @pl.when(jnp.logical_not(lower))
    def _():
        for i in range(chips):
            signal(group=i)

    keep = pltpu.make_async_copy(
        cache.at[:, pl.ds(pl.multiple_of(rank * span, span), span), :],
        cache_out.at[pl.ds(rank * pairs, pairs)],
        local_sem,
    )
    keep.start()
    for offset in offsets:
        if FIRST(*offset):
            cache_copy(tensor_peer(*offset)).start()
    for load in loads[6:]:
        load.wait()
    others = stream.at[pl.ds(0, seqs - 1)]
    remote(others, others, stream_send, stream_recv, tensor=rank).wait_recv()

    def scale_part(at):
        for c in range(heads):
            tile = raw[at, c].astype(jnp.float32)
            scaled[at * pieces + c // own_blocks, c % own_blocks] = (tile * gain[pl.ds(at * heads + c, 1), :]).astype(
                jnp.bfloat16
            )

    for k in range(seqs):
        stream_rows[k * ROWS : (k + 1) * ROWS, :] = stream[k].astype(jnp.float32)
    for c in range(heads):
        raw[part, c] = stream_rows[pl.ds(c, seqs, stride=ROWS), :].astype(jnp.bfloat16)
    each(parts, lambda i: raw_copy(part_peer(i)).start())
    for offset in offsets:
        if not FIRST(*offset):
            cache_copy(tensor_peer(*offset)).start()
    scale_part(part)

    @pl.when(lower)
    def _():
        pl.semaphore_wait(barrier, chips)
        signal(group=groups - 1 - mine)

    @pl.when(jnp.logical_not(lower))
    def _():
        pl.semaphore_wait(barrier, 1)

    def send_part(at):
        for piece in range(pieces):
            to = at * pieces + piece

            @pl.when(to != mine)
            def _():
                column_copy(to).start()

    send_part(part)
    own_columns = pltpu.make_async_copy(
        scaled.at[mine], columns.at[mine], column_recv.at[batch]
    )
    other_parts = raw.at[pl.ds(0, parts - 1)]
    remote(other_parts, other_parts, raw_send, raw_recv, group=mine).wait_recv()
    for i in range(1, parts):
        scale_part(part_peer(i))
    for i in range(1, parts):
        send_part(part_peer(i))
    own_columns.start()

    def choose(to, target, at):
        rows = pl.ds(pl.multiple_of(to * seqs, seqs), seqs)
        both = columns[to, own_blocks].astype(jnp.float32)
        swapped = pltpu.roll(both, LANES // 2, 1)
        for k in range(2):
            near, far = (both, swapped) if k == 0 else (swapped, both)
            route = jnp.where(lane < LANES // 2, near, far)
            route = jnp.concatenate([route] * (hidden // LANES), axis=1)
            for q, source in enumerate((gate_all, up_all)):
                value = source[0, rows, :]
                for e in range(1, experts):
                    value = jnp.where(route == float(e), source[e, rows, :], value)
                target[at, 2 * k + q] = value.astype(target.dtype)

    def pair_copy(b):
        at = pl.ds(b * half, half)
        return remote(
            pair_out.at[at],
            pair_in.at[at],
            pair_send.at[b],
            pair_recv.at[b],
            group=2 * chip + 1 - core,
        )

    def expert_batch(b):
        some = columns.at[pl.ds(b * chips, chips)]
        remote(some, some, column_send, column_recv.at[b], group=mine).wait_recv()
        rows = pl.ds(b * chips * seqs, chips * seqs)
        for c in range(own_blocks):
            tokens[rows, c * LANES : (c + 1) * LANES] = (
                columns[pl.ds(b * chips, chips), c]
                .astype(jnp.float32)
                .reshape(chips * seqs, LANES)
                .astype(jnp.bfloat16)
            )
        for e in range(experts):
            gate_all[e, rows, :] = jnp.dot(
                tokens[rows, :], gate_w[e], preferred_element_type=jnp.float32
            )
            up_all[e, rows, :] = jnp.dot(
                tokens[rows, :], up_w[e], preferred_element_type=jnp.float32
            )

        def for_pair(i, carry):
            choose(2 * i + 1 - core, pair_out, i)
            return carry

        def for_own(i, carry):
            choose(2 * i + core, pair_own, i)
            return carry

        lax.fori_loop(b * half, (b + 1) * half, for_pair, 0)
        pair_copy(b).start()
        lax.fori_loop(b * half, (b + 1) * half, for_own, 0)
        pair_copy(b).wait_recv()
        first = jnp.where(chip // half == b, half // 2, 0)
        order = [
            b * half + lax.rem(chip + first + i, half)
            for i in sorted(range(half), key=lambda i: min(i, half - i))
        ]

        def send_sum(to):
            @pl.when(to != chip)
            def _():
                sum_copy(to).start()

        for n, to in enumerate(order):
            partial[to] = (pair_own[to] + pair_in[to].astype(jnp.float32)).astype(jnp.bfloat16)
            if n:
                send_sum(order[n - 1])
        send_sum(order[-1])

    expert_batch(0)

    total = jnp.zeros((seqs, LANES), jnp.float32)
    for c in range(blocks):
        value = raw[c // heads, c % heads]
        updated_out[:, c * LANES : (c + 1) * LANES] = value
        value = value.astype(jnp.float32)
        total = total + value * value
    scale = lax.rsqrt(jnp.sum(total, axis=1, keepdims=True) / cols + 1e-05)
    for c in range(blocks):
        value = raw[c // heads, c % heads].astype(jnp.float32)
        normed[:, c * LANES : (c + 1) * LANES] = (value * scale * gain[c : c + 1, :]).astype(
            jnp.bfloat16
        )
    logits = lax.dot_general(normed[...], router[...], NT, preferred_element_type=jnp.float32)
    expert_id = lax.broadcasted_iota(jnp.int32, (seqs, experts), 1)
    chosen = [
        jnp.sum(
            jnp.where(routes[k][:, :1] == expert_id, logits, 0.0), axis=1, keepdims=True
        )
        for k in range(2)
    ]
    gate_weights = [
        1.0 / (1.0 + jnp.exp(chosen[1] - chosen[0])),
        1.0 / (1.0 + jnp.exp(chosen[0] - chosen[1])),
    ]

    expert_batch(1)
    arrived[chip] = partial[chip]
    other_sums = arrived.at[pl.ds(0, chips - 1)]
    remote(other_sums, other_sums, sum_send, sum_recv, group=mine).wait_recv()
    units = []
    for k in range(2):
        sums = []
        for q in range(2):
            value = arrived[0, 2 * k + q].astype(jnp.float32)
            for s in range(1, chips):
                value = value + arrived[s, 2 * k + q].astype(jnp.float32)
            sums.append(value * scale)
        silu = sums[0] / (1.0 + jnp.exp(-sums[0]))
        units.append(gate_weights[k] * silu * sums[1])
    for s in range(seqs):
        hidden_out[s] = jnp.concatenate([unit[s : s + 1] for unit in units], axis=0).astype(
            jnp.bfloat16
        )

    remote(others, others, stream_send, stream_recv, tensor=rank).wait_send()
    remote(other_parts, other_parts, raw_send, raw_recv, group=mine).wait_send()
    for b in range(2):
        pair_copy(b).wait_send()
    remote(other_sums, other_sums, sum_send, sum_recv, group=mine).wait_send()
    most = columns.at[pl.ds(0, groups - 1)]
    remote(most, most, column_send, column_recv.at[0], group=mine).wait_send()

    most_cache = cache_out.at[pl.ds(0, (tensors - 1) * pairs)]
    remote(most_cache, most_cache, cache_send, cache_recv, tensor=rank).wait_send()
    keep.wait()
    remote(most_cache, most_cache, cache_send, cache_recv, tensor=rank).wait_recv()


def write_out(updated, hidden_units, cache, updated_hbm, hidden_hbm, cache_hbm, sems):
    copies = [
        pltpu.make_async_copy(source, target, sems.at[k])
        for k, (source, target) in enumerate(
            ((cache, cache_hbm), (updated, updated_hbm), (hidden_units, hidden_hbm))
        )
    ]
    for copy in copies:
        copy.start()
    for copy in copies:
        copy.wait()


def body(
    groups,
    tensors,
    key_value_cache,
    queries,
    fresh_key_value,
    lengths,
    residual,
    norm_gain,
    router_weight,
    routing,
    expert_gate,
    expert_up,
):
    pairs, slots, width = key_value_cache.shape
    seqs, q_heads, head = queries.shape
    kv_heads = fresh_key_value.shape[1]
    cols = residual.shape[1]
    experts, own_cols, hidden = expert_gate.shape
    span = slots // tensors
    parts = tensors // seqs
    heads = cols // parts // head
    bf16, f32, i32 = jnp.bfloat16, jnp.float32, jnp.int32
    dma = pltpu.SemaphoreType.DMA
    hbm = pl.BlockSpec(memory_space=pltpu.HBM)
    vmem = pl.BlockSpec(memory_space=pltpu.VMEM)
    updated, hidden_units, new_cache = pl.pallas_call(
        functools.partial(kernel, (groups, tensors, span)),
        out_shape=(
            pltpu.VMEM((seqs, cols), bf16),
            pltpu.VMEM((seqs, 2, hidden), bf16),
            pltpu.VMEM((seqs * kv_heads, span, width), bf16),
        ),
        in_specs=[hbm] * 10,
        out_specs=(vmem, vmem, vmem),
        scratch_shapes=[
            pltpu.SMEM((seqs,), i32),
            pltpu.SMEM((2, seqs), i32),
            pltpu.VMEM((pairs, slots, width), bf16),
            pltpu.VMEM((q_heads, head), bf16),
            pltpu.VMEM((kv_heads, width), bf16),
            pltpu.VMEM((seqs, cols), bf16),
            pltpu.VMEM((cols // LANES, LANES), f32),
            pltpu.VMEM((experts, cols), bf16),
            pltpu.VMEM(expert_gate.shape, bf16),
            pltpu.VMEM(expert_up.shape, bf16),
            pltpu.VMEM((ROWS * seqs, LANES), f32),
            pltpu.VMEM((seqs, ROWS, LANES), bf16),
            pltpu.VMEM((seqs * ROWS, LANES), f32),
            pltpu.VMEM((parts, heads, seqs, LANES), bf16),
            pltpu.VMEM((groups, own_cols // LANES + 1, seqs, LANES), bf16),
            pltpu.VMEM((seqs, cols), bf16),
            pltpu.VMEM((groups, own_cols // LANES + 1, seqs, LANES), bf16),
            pltpu.VMEM((groups * seqs, own_cols), bf16),
            pltpu.VMEM((2, seqs, LANES), i32),
            pltpu.VMEM((experts, groups * seqs, hidden), f32),
            pltpu.VMEM((experts, groups * seqs, hidden), f32),
            pltpu.VMEM((groups // 2, 4, seqs, hidden), bf16),
            pltpu.VMEM((groups // 2, 4, seqs, hidden), bf16),
            pltpu.VMEM((groups // 2, 4, seqs, hidden), f32),
            pltpu.VMEM((groups // 2, 4, seqs, hidden), bf16),
            pltpu.VMEM((groups // 2, 4, seqs, hidden), bf16),
            dma((10,)),
        ]
        + [dma(())] * 8
        + [dma((2,))] * 3
        + [dma(())] * 2,
        compiler_params=pltpu.CompilerParams(
            collective_id=0, has_side_effects=True
        ),
    )(
        lengths,
        routing.T,
        key_value_cache,
        queries,
        fresh_key_value,
        residual,
        norm_gain.reshape(cols // LANES, LANES),
        router_weight.T,
        expert_gate,
        expert_up,
    )
    updated, hidden_units, new_cache = pl.pallas_call(
        write_out,
        out_shape=(
            jax.ShapeDtypeStruct(updated.shape, bf16),
            jax.ShapeDtypeStruct(hidden_units.shape, bf16),
            jax.ShapeDtypeStruct(new_cache.shape, bf16),
        ),
        in_specs=[vmem] * 3,
        out_specs=(hbm,) * 3,
        scratch_shapes=[dma((3,))],
        compiler_params=pltpu.CompilerParams(vmem_limit_bytes=4 << 20),
    )(updated, hidden_units, new_cache)
    return (
        updated,
        hidden_units,
        new_cache.reshape(seqs, kv_heads, span, width),
    )


def solution(mesh):
    in_specs = (
        P(("group", "tensor"), None, None),
        P("group", None, None),
        P("group", None, None),
        P("group"),
        P("group", None),
        P(),
        P(),
        P("group", None),
        P(None, "group", "tensor"),
        P(None, "group", "tensor"),
    )
    out_specs = (P("group", None), P("group", None, "tensor"), P("group", None, "tensor", None))
    return jax.shard_map(
        functools.partial(body, mesh.shape["group"], mesh.shape["tensor"]),
        mesh=mesh,
        in_specs=in_specs,
        out_specs=out_specs,
        check_vma=False,
    )
```

```python
import functools
import math

import jax
import jax.numpy as jnp
from jax import lax
from jax.experimental import pallas as pl
from jax.experimental.pallas import tpu as pltpu
from jax.sharding import PartitionSpec as P

MESH = pl.DeviceIdType.MESH
LANES = 128
ROWS = 16
NT = (((1,), (1,)), ((), ()))


EARLY = 2


def goes_first(down, along):
    return along == 0 or down in (0, 1, 7) or (down in (2, 6) and along == 2)


def kernel(
    dims,
    lengths_hbm,
    routing_hbm,
    cache_hbm,
    queries_hbm,
    fresh_hbm,
    residual_hbm,
    gain_hbm,
    router_hbm,
    gate_hbm,
    up_hbm,
    updated_out,
    hidden_out,
    cache_out,
    lengths,
    routing,
    cache,
    queries,
    fresh,
    residual,
    gain,
    router,
    gate_w,
    up_w,
    residual_rows,
    stream,
    stream_rows,
    raw,
    scaled,
    normed,
    columns,
    tokens,
    routes,
    gate_all,
    up_all,
    pair_out,
    pair_in,
    pair_own,
    partial,
    arrived,
    load_sem,
    local_sem,
    stream_send,
    stream_recv,
    raw_send,
    raw_recv,
    cache_send,
    cache_recv,
    column_send,
    column_recv,
    pair_send,
    pair_recv,
    sum_send,
    sum_recv,
):
    groups, tensors, span = dims
    mine = lax.axis_index("group")
    rank = lax.axis_index("tensor")
    pairs, slots, width = cache.shape
    head = width // 2
    seqs, cols = updated_out.shape
    parts = tensors // seqs
    seq = rank // parts
    part = lax.rem(rank, parts)
    heads = cols // parts // head
    share = heads // pairs
    blocks = cols // LANES
    own_blocks = blocks // groups
    pieces = groups // parts
    experts = gate_w.shape[0]
    hidden = gate_w.shape[2]
    chips = groups // 2
    chip = mine // 2
    core = lax.rem(mine, 2)
    lower = mine < chips
    batches = ((0, EARLY), (EARLY, chips))
    batch = jnp.where(chip < EARLY, 0, 1)

    def group_peer(i):
        return lax.rem(mine + i, groups)

    def seq_peer(i):
        return lax.rem(seq + i, seqs)

    def part_peer(i):
        return lax.rem(part + i, parts)

    def chip_peer(i):
        return lax.rem(chip + i, chips)

    def tensor_peer(down, along):
        return lax.rem(seq + down, seqs) * parts + lax.rem(part + along, parts)

    offsets = sorted(
        ((down, along) for down in range(seqs) for along in range(parts) if down or along),
        key=lambda o: -min(o[0], seqs - o[0]) - min(o[1], parts - o[1]),
    )

    def remote(source, target, send, recv, **to):
        return pltpu.make_async_remote_copy(
            src_ref=source,
            dst_ref=target,
            send_sem=send,
            recv_sem=recv,
            device_id=to,
            device_id_type=MESH,
        )

    def cache_copy(to):
        return remote(
            cache.at[:, pl.ds(pl.multiple_of(to * span, span), span), :],
            cache_out.at[pl.ds(rank * pairs, pairs)],
            cache_send,
            cache_recv,
            tensor=to,
        )

    def stream_copy(to):
        return remote(
            stream.at[seq], stream.at[seq], stream_send, stream_recv, tensor=to * parts + part
        )

    def raw_copy(to):
        return remote(raw.at[part], raw.at[part], raw_send, raw_recv, tensor=seq * parts + to)

    def column_copy(to):
        return remote(
            scaled.at[to],
            columns.at[mine],
            column_send,
            column_recv.at[batch],
            group=to,
        )

    def sum_copy(to):
        return remote(
            partial.at[to], arrived.at[chip], sum_send, sum_recv, group=2 * to + core
        )

    def signal(**to):
        pl.semaphore_signal(barrier, inc=1, device_id=to, device_id_type=MESH)

    def each(count, step):
        def go(i, carry):
            step(i)
            return carry

        lax.fori_loop(1, count, go, 0)

    loads = [
        pltpu.make_async_copy(source, target, load_sem.at[k])
        for k, (source, target) in enumerate(
            (
                (cache_hbm, cache),
                (lengths_hbm, lengths),
                (queries_hbm.at[seq], queries),
                (fresh_hbm.at[seq], fresh),
                (residual_hbm, residual),
                (routing_hbm, routing),
                (gain_hbm, gain),
                (router_hbm, router),
                (gate_hbm, gate_w),
                (up_hbm, up_w),
            )
        )
    ]
    for load in loads:
        load.start()

    barrier = pltpu.get_barrier_semaphore()
    for offset in offsets:
        signal(tensor=tensor_peer(*offset))

    for load in loads[:6]:
        load.wait()

    length = lengths[seq]
    fresh_rows = fresh[...].astype(jnp.float32)
    row_id = lax.broadcasted_iota(jnp.int32, fresh_rows.shape, 0)
    chunk = 128
    for p in range(pairs):
        own_row = jnp.sum(
            jnp.where(row_id == part * pairs + p, fresh_rows, 0.0), axis=0, keepdims=True
        )

        def place(c, carry, p=p, own_row=own_row):
            at = pl.ds(pl.multiple_of(c * chunk, chunk), chunk)
            slot_id = lax.broadcasted_iota(jnp.int32, (chunk, width), 0) + c * chunk
            cache[p, at, :] = jnp.where(
                slot_id == length, own_row, cache[p, at, :].astype(jnp.float32)
            ).astype(jnp.bfloat16)
            return carry

        lax.fori_loop(0, slots // chunk, place, 0)

    pick = (
        lax.broadcasted_iota(jnp.int32, (ROWS, queries.shape[0]), 1)
        == lax.broadcasted_iota(jnp.int32, (ROWS, queries.shape[0]), 0) + part * heads
    )
    own_queries = jnp.dot(
        pick.astype(jnp.float32).astype(jnp.bfloat16),
        queries[...],
        preferred_element_type=jnp.float32,
    ).astype(jnp.bfloat16)
    visible = lax.broadcasted_iota(jnp.int32, (ROWS, slots), 1) <= length
    out_row = lax.broadcasted_iota(jnp.int32, (ROWS, head), 0)
    attention = None
    for p in range(pairs):
        scores = lax.dot_general(
            own_queries, cache[p, :, :head], NT, preferred_element_type=jnp.float32
        ) * (1.0 / math.sqrt(head))
        scores = jnp.where(visible, scores, -1e30)
        peak = jnp.max(scores, axis=1, keepdims=True)
        weights = jnp.where(visible, jnp.exp(scores - peak), 0.0)
        denominator = jnp.sum(weights, axis=1, keepdims=True)
        weighted = jnp.dot(
            weights.astype(jnp.bfloat16), cache[p, :, head:], preferred_element_type=jnp.float32
        )
        result = weighted / denominator
        attention = result if p == 0 else jnp.where(out_row < p * share, attention, result)

    residual_rows[...] = jnp.zeros_like(residual_rows)
    for c in range(heads):
        at = pl.ds(pl.multiple_of(part * heads * LANES + c * LANES, LANES), LANES)
        residual_rows[c * seqs : (c + 1) * seqs, :] = residual[:, at].astype(jnp.float32)
    own_residual = residual_rows[pl.ds(seq, ROWS, stride=seqs), :]
    stream[seq] = (own_residual + attention).astype(jnp.bfloat16)

    sublane = lax.broadcasted_iota(jnp.int32, (seqs, LANES), 0)
    for k in range(routing.shape[0]):
        value = jnp.zeros((seqs, LANES), jnp.int32)
        for s in range(seqs):
            value = jnp.where(sublane == s, routing[k, s], value)
        routes[k] = value
    lane = lax.broadcasted_iota(jnp.int32, (seqs, LANES), 1)
    both = jnp.where(lane < LANES // 2, routes[0], routes[1])
    for to in range(groups):
        scaled[to, own_blocks] = both.astype(jnp.float32).astype(jnp.bfloat16)

    pl.semaphore_wait(barrier, tensors - 1 + jnp.where(lower, 0, chips))
    for i in sorted(range(1, seqs), key=lambda i: -min(i, seqs - i)):
        stream_copy(seq_peer(i)).start()

    @pl.when(lower)
    def _():
        for i in range(chips, groups):
            signal(group=i)

    @pl.when(jnp.logical_not(lower))
    def _():
        for i in range(chips):
            signal(group=i)

    keep = pltpu.make_async_copy(
        cache.at[:, pl.ds(pl.multiple_of(rank * span, span), span), :],
        cache_out.at[pl.ds(rank * pairs, pairs)],
        local_sem,
    )
    keep.start()
    for offset in offsets:
        if goes_first(*offset):
            cache_copy(tensor_peer(*offset)).start()
    for load in loads[6:]:
        load.wait()
    others = stream.at[pl.ds(0, seqs - 1)]
    remote(others, others, stream_send, stream_recv, tensor=rank).wait_recv()

    def scale_part(at):
        for c in range(heads):
            tile = raw[at, c].astype(jnp.float32)
            scaled[at * pieces + c // own_blocks, c % own_blocks] = (tile * gain[pl.ds(at * heads + c, 1), :]).astype(
                jnp.bfloat16
            )

    for k in range(seqs):
        stream_rows[k * ROWS : (k + 1) * ROWS, :] = stream[k].astype(jnp.float32)
    for c in range(heads):
        raw[part, c] = stream_rows[pl.ds(c, seqs, stride=ROWS), :].astype(jnp.bfloat16)
    each(parts, lambda i: raw_copy(part_peer(i)).start())
    for offset in offsets:
        if not goes_first(*offset):
            cache_copy(tensor_peer(*offset)).start()
    scale_part(part)

    @pl.when(lower)
    def _():
        pl.semaphore_wait(barrier, chips)
        signal(group=groups - 1 - mine)

    @pl.when(jnp.logical_not(lower))
    def _():
        pl.semaphore_wait(barrier, 1)

    def send_part(at):
        for piece in range(pieces):
            to = at * pieces + piece

            @pl.when(to != mine)
            def _():
                column_copy(to).start()

    send_part(part)
    own_columns = pltpu.make_async_copy(
        scaled.at[mine], columns.at[mine], column_recv.at[batch]
    )
    other_parts = raw.at[pl.ds(0, parts - 1)]
    remote(other_parts, other_parts, raw_send, raw_recv, group=mine).wait_recv()
    for i in range(1, parts):
        scale_part(part_peer(i))
    for i in range(1, parts):
        send_part(part_peer(i))
    own_columns.start()

    def choose(to, target, at):
        rows = pl.ds(pl.multiple_of(to * seqs, seqs), seqs)
        both = columns[to, own_blocks].astype(jnp.float32)
        swapped = pltpu.roll(both, LANES // 2, 1)
        for k in range(2):
            near, far = (both, swapped) if k == 0 else (swapped, both)
            route = jnp.where(lane < LANES // 2, near, far)
            route = jnp.concatenate([route] * (hidden // LANES), axis=1)
            for q, source in enumerate((gate_all, up_all)):
                value = source[0, rows, :]
                for e in range(1, experts):
                    value = jnp.where(route == float(e), source[e, rows, :], value)
                target[at, 2 * k + q] = value.astype(target.dtype)

    def pair_copy(b):
        first, last = batches[b]
        at = pl.ds(first, last - first)
        return remote(
            pair_out.at[at],
            pair_in.at[at],
            pair_send.at[b],
            pair_recv.at[b],
            group=2 * chip + 1 - core,
        )

    def expert_batch(b):
        first, last = batches[b]
        count = last - first
        some = columns.at[pl.ds(2 * first, 2 * count)]
        remote(some, some, column_send, column_recv.at[b], group=mine).wait_recv()
        rows = pl.ds(2 * first * seqs, 2 * count * seqs)
        for c in range(own_blocks):
            tokens[rows, c * LANES : (c + 1) * LANES] = (
                columns[pl.ds(2 * first, 2 * count), c]
                .astype(jnp.float32)
                .reshape(2 * count * seqs, LANES)
                .astype(jnp.bfloat16)
            )
        for e in range(experts):
            gate_all[e, rows, :] = jnp.dot(
                tokens[rows, :], gate_w[e], preferred_element_type=jnp.float32
            )
            up_all[e, rows, :] = jnp.dot(
                tokens[rows, :], up_w[e], preferred_element_type=jnp.float32
            )

        def for_pair(i, carry):
            choose(2 * i + 1 - core, pair_out, i)
            return carry

        def for_own(i, carry):
            choose(2 * i + core, pair_own, i)
            return carry

        lax.fori_loop(first, last, for_pair, 0)
        pair_copy(b).start()
        lax.fori_loop(first, last, for_own, 0)
        pair_copy(b).wait_recv()
        order = list(range(first, last))

        def send_sum(to):
            @pl.when(to != chip)
            def _():
                sum_copy(to).start()

        for n, to in enumerate(order):
            partial[to] = (pair_own[to] + pair_in[to].astype(jnp.float32)).astype(jnp.bfloat16)
            if n:
                send_sum(order[n - 1])
        send_sum(order[-1])

    expert_batch(0)

    total = jnp.zeros((seqs, LANES), jnp.float32)
    for c in range(blocks):
        value = raw[c // heads, c % heads]
        updated_out[:, c * LANES : (c + 1) * LANES] = value
        value = value.astype(jnp.float32)
        total = total + value * value
    scale = lax.rsqrt(jnp.sum(total, axis=1, keepdims=True) / cols + 1e-05)
    for c in range(blocks):
        value = raw[c // heads, c % heads].astype(jnp.float32)
        normed[:, c * LANES : (c + 1) * LANES] = (value * scale * gain[c : c + 1, :]).astype(
            jnp.bfloat16
        )
    logits = lax.dot_general(normed[...], router[...], NT, preferred_element_type=jnp.float32)
    expert_id = lax.broadcasted_iota(jnp.int32, (seqs, experts), 1)
    chosen = [
        jnp.sum(
            jnp.where(routes[k][:, :1] == expert_id, logits, 0.0), axis=1, keepdims=True
        )
        for k in range(2)
    ]
    gate_weights = [
        1.0 / (1.0 + jnp.exp(chosen[1] - chosen[0])),
        1.0 / (1.0 + jnp.exp(chosen[0] - chosen[1])),
    ]

    expert_batch(1)
    arrived[chip] = partial[chip]
    other_sums = arrived.at[pl.ds(0, chips - 1)]
    remote(other_sums, other_sums, sum_send, sum_recv, group=mine).wait_recv()
    units = []
    for k in range(2):
        sums = []
        for q in range(2):
            value = arrived[0, 2 * k + q].astype(jnp.float32)
            for s in range(1, chips):
                value = value + arrived[s, 2 * k + q].astype(jnp.float32)
            sums.append(value * scale)
        silu = sums[0] / (1.0 + jnp.exp(-sums[0]))
        units.append(gate_weights[k] * silu * sums[1])
    for s in range(seqs):
        hidden_out[s] = jnp.concatenate([unit[s : s + 1] for unit in units], axis=0).astype(
            jnp.bfloat16
        )

    remote(others, others, stream_send, stream_recv, tensor=rank).wait_send()
    remote(other_parts, other_parts, raw_send, raw_recv, group=mine).wait_send()
    for b in range(2):
        pair_copy(b).wait_send()
    remote(other_sums, other_sums, sum_send, sum_recv, group=mine).wait_send()
    most = columns.at[pl.ds(0, groups - 1)]
    remote(most, most, column_send, column_recv.at[0], group=mine).wait_send()

    most_cache = cache_out.at[pl.ds(0, (tensors - 1) * pairs)]
    remote(most_cache, most_cache, cache_send, cache_recv, tensor=rank).wait_send()
    keep.wait()
    remote(most_cache, most_cache, cache_send, cache_recv, tensor=rank).wait_recv()


def write_out(updated, hidden_units, cache, updated_hbm, hidden_hbm, cache_hbm, sems):
    copies = [
        pltpu.make_async_copy(source, target, sems.at[k])
        for k, (source, target) in enumerate(
            ((cache, cache_hbm), (updated, updated_hbm), (hidden_units, hidden_hbm))
        )
    ]
    for copy in copies:
        copy.start()
    for copy in copies:
        copy.wait()


def body(
    groups,
    tensors,
    key_value_cache,
    queries,
    fresh_key_value,
    lengths,
    residual,
    norm_gain,
    router_weight,
    routing,
    expert_gate,
    expert_up,
):
    pairs, slots, width = key_value_cache.shape
    seqs, q_heads, head = queries.shape
    kv_heads = fresh_key_value.shape[1]
    cols = residual.shape[1]
    experts, own_cols, hidden = expert_gate.shape
    span = slots // tensors
    parts = tensors // seqs
    heads = cols // parts // head
    bf16, f32, i32 = jnp.bfloat16, jnp.float32, jnp.int32
    dma = pltpu.SemaphoreType.DMA
    hbm = pl.BlockSpec(memory_space=pltpu.HBM)
    vmem = pl.BlockSpec(memory_space=pltpu.VMEM)
    updated, hidden_units, new_cache = pl.pallas_call(
        functools.partial(kernel, (groups, tensors, span)),
        out_shape=(
            pltpu.VMEM((seqs, cols), bf16),
            pltpu.VMEM((seqs, 2, hidden), bf16),
            pltpu.VMEM((seqs * kv_heads, span, width), bf16),
        ),
        in_specs=[hbm] * 10,
        out_specs=(vmem, vmem, vmem),
        scratch_shapes=[
            pltpu.SMEM((seqs,), i32),
            pltpu.SMEM((2, seqs), i32),
            pltpu.VMEM((pairs, slots, width), bf16),
            pltpu.VMEM((q_heads, head), bf16),
            pltpu.VMEM((kv_heads, width), bf16),
            pltpu.VMEM((seqs, cols), bf16),
            pltpu.VMEM((cols // LANES, LANES), f32),
            pltpu.VMEM((experts, cols), bf16),
            pltpu.VMEM(expert_gate.shape, bf16),
            pltpu.VMEM(expert_up.shape, bf16),
            pltpu.VMEM(((ROWS + 1) * seqs, LANES), f32),
            pltpu.VMEM((seqs, ROWS, LANES), bf16),
            pltpu.VMEM((seqs * ROWS, LANES), f32),
            pltpu.VMEM((parts, heads, seqs, LANES), bf16),
            pltpu.VMEM((groups, own_cols // LANES + 1, seqs, LANES), bf16),
            pltpu.VMEM((seqs, cols), bf16),
            pltpu.VMEM((groups, own_cols // LANES + 1, seqs, LANES), bf16),
            pltpu.VMEM((groups * seqs, own_cols), bf16),
            pltpu.VMEM((2, seqs, LANES), i32),
            pltpu.VMEM((experts, groups * seqs, hidden), f32),
            pltpu.VMEM((experts, groups * seqs, hidden), f32),
            pltpu.VMEM((groups // 2, 4, seqs, hidden), bf16),
            pltpu.VMEM((groups // 2, 4, seqs, hidden), bf16),
            pltpu.VMEM((groups // 2, 4, seqs, hidden), f32),
            pltpu.VMEM((groups // 2, 4, seqs, hidden), bf16),
            pltpu.VMEM((groups // 2, 4, seqs, hidden), bf16),
            dma((10,)),
        ]
        + [dma(())] * 8
        + [dma((2,))] * 3
        + [dma(())] * 2,
        compiler_params=pltpu.CompilerParams(
            collective_id=0, has_side_effects=True
        ),
    )(
        lengths,
        routing.T,
        key_value_cache,
        queries,
        fresh_key_value,
        residual,
        norm_gain.reshape(cols // LANES, LANES),
        router_weight.T,
        expert_gate,
        expert_up,
    )
    updated, hidden_units, new_cache = pl.pallas_call(
        write_out,
        out_shape=(
            jax.ShapeDtypeStruct(updated.shape, bf16),
            jax.ShapeDtypeStruct(hidden_units.shape, bf16),
            jax.ShapeDtypeStruct(new_cache.shape, bf16),
        ),
        in_specs=[vmem] * 3,
        out_specs=(hbm,) * 3,
        scratch_shapes=[dma((3,))],
        compiler_params=pltpu.CompilerParams(vmem_limit_bytes=4 << 20),
    )(updated, hidden_units, new_cache)
    return (
        updated,
        hidden_units,
        new_cache.reshape(seqs, kv_heads, span, width),
    )


def solution(mesh):
    in_specs = (
        P(("group", "tensor"), None, None),
        P("group", None, None),
        P("group", None, None),
        P("group"),
        P("group", None),
        P(),
        P(),
        P("group", None),
        P(None, "group", "tensor"),
        P(None, "group", "tensor"),
    )
    out_specs = (P("group", None), P("group", None, "tensor"), P("group", None, "tensor", None))
    return jax.shard_map(
        functools.partial(body, mesh.shape["group"], mesh.shape["tensor"]),
        mesh=mesh,
        in_specs=in_specs,
        out_specs=out_specs,
        check_vma=False,
    )
```

```python
import functools
import math

import jax
import jax.numpy as jnp
from jax import lax
from jax.experimental import pallas as pl
from jax.experimental.pallas import tpu as pltpu
from jax.sharding import PartitionSpec as P

MESH = pl.DeviceIdType.MESH
LANES = 128
ROWS = 16
NT = (((1,), (1,)), ((), ()))


EARLY = 2


def goes_first(down, along):
    return along == 0 or down in (0, 1, 7) or (down in (2, 6) and along == 2)


def kernel(
    dims,
    lengths_hbm,
    routing_hbm,
    cache_hbm,
    queries_hbm,
    fresh_hbm,
    residual_hbm,
    gain_hbm,
    router_hbm,
    gate_hbm,
    up_hbm,
    updated_out,
    hidden_out,
    cache_out,
    lengths,
    routing,
    cache,
    queries,
    fresh,
    residual,
    gain,
    router,
    gate_w,
    up_w,
    residual_rows,
    stream,
    stream_rows,
    raw,
    scaled,
    normed,
    columns,
    tokens,
    routes,
    gate_all,
    up_all,
    pair_out,
    pair_in,
    pair_own,
    partial,
    arrived,
    load_sem,
    local_sem,
    stream_send,
    stream_recv,
    raw_send,
    raw_recv,
    cache_send,
    cache_recv,
    column_send,
    column_recv,
    pair_send,
    pair_recv,
    sum_send,
    sum_recv,
):
    groups, tensors, span = dims
    mine = lax.axis_index("group")
    rank = lax.axis_index("tensor")
    pairs, slots, width = cache.shape
    head = width // 2
    seqs, cols = updated_out.shape
    parts = tensors // seqs
    seq = rank // parts
    part = lax.rem(rank, parts)
    heads = cols // parts // head
    share = heads // pairs
    blocks = cols // LANES
    own_blocks = blocks // groups
    pieces = groups // parts
    experts = gate_w.shape[0]
    hidden = gate_w.shape[2]
    chips = groups // 2
    chip = mine // 2
    core = lax.rem(mine, 2)
    lower = mine < chips
    batches = ((0, EARLY), (EARLY, chips))
    batch = jnp.where(chip < EARLY, 0, 1)

    def group_peer(i):
        return lax.rem(mine + i, groups)

    def seq_peer(i):
        return lax.rem(seq + i, seqs)

    def part_peer(i):
        return lax.rem(part + i, parts)

    def chip_peer(i):
        return lax.rem(chip + i, chips)

    def tensor_peer(down, along):
        return lax.rem(seq + down, seqs) * parts + lax.rem(part + along, parts)

    offsets = sorted(
        ((down, along) for down in range(seqs) for along in range(parts) if down or along),
        key=lambda o: -min(o[0], seqs - o[0]) - min(o[1], parts - o[1]),
    )

    def remote(source, target, send, recv, **to):
        return pltpu.make_async_remote_copy(
            src_ref=source,
            dst_ref=target,
            send_sem=send,
            recv_sem=recv,
            device_id=to,
            device_id_type=MESH,
        )

    def cache_copy(to):
        return remote(
            cache.at[:, pl.ds(pl.multiple_of(to * span, span), span), :],
            cache_out.at[pl.ds(rank * pairs, pairs)],
            cache_send,
            cache_recv,
            tensor=to,
        )

    def stream_copy(to):
        return remote(
            stream.at[seq], stream.at[seq], stream_send, stream_recv, tensor=to * parts + part
        )

    def raw_copy(to):
        return remote(raw.at[part], raw.at[part], raw_send, raw_recv, tensor=seq * parts + to)

    def column_copy(to):
        return remote(
            scaled.at[to],
            columns.at[mine],
            column_send,
            column_recv.at[batch],
            group=to,
        )

    def sum_copy(to):
        return remote(
            partial.at[to], arrived.at[chip], sum_send, sum_recv, group=2 * to + core
        )

    def signal(**to):
        pl.semaphore_signal(barrier, inc=1, device_id=to, device_id_type=MESH)

    def each(count, step):
        def go(i, carry):
            step(i)
            return carry

        lax.fori_loop(1, count, go, 0)

    barrier = pltpu.get_barrier_semaphore()
    for offset in offsets:
        signal(tensor=tensor_peer(*offset))

    loads = [
        pltpu.make_async_copy(source, target, load_sem.at[k])
        for k, (source, target) in enumerate(
            (
                (cache_hbm, cache),
                (lengths_hbm, lengths),
                (queries_hbm.at[seq], queries),
                (fresh_hbm.at[seq], fresh),
                (residual_hbm, residual),
                (routing_hbm, routing),
                (gain_hbm, gain),
                (router_hbm, router),
                (gate_hbm, gate_w),
                (up_hbm, up_w),
            )
        )
    ]
    for load in loads[:6]:
        load.start()

    for load in loads[:6]:
        load.wait()
    for load in loads[6:]:
        load.start()

    length = lengths[seq]
    fresh_rows = fresh[...].astype(jnp.float32)
    row_id = lax.broadcasted_iota(jnp.int32, fresh_rows.shape, 0)
    chunk = 128
    for p in range(pairs):
        own_row = jnp.sum(
            jnp.where(row_id == part * pairs + p, fresh_rows, 0.0), axis=0, keepdims=True
        )

        def place(c, carry, p=p, own_row=own_row):
            at = pl.ds(pl.multiple_of(c * chunk, chunk), chunk)
            slot_id = lax.broadcasted_iota(jnp.int32, (chunk, width), 0) + c * chunk
            cache[p, at, :] = jnp.where(
                slot_id == length, own_row, cache[p, at, :].astype(jnp.float32)
            ).astype(jnp.bfloat16)
            return carry

        lax.fori_loop(0, slots // chunk, place, 0)

    pick = (
        lax.broadcasted_iota(jnp.int32, (ROWS, queries.shape[0]), 1)
        == lax.broadcasted_iota(jnp.int32, (ROWS, queries.shape[0]), 0) + part * heads
    )
    own_queries = jnp.dot(
        pick.astype(jnp.float32).astype(jnp.bfloat16),
        queries[...],
        preferred_element_type=jnp.float32,
    ).astype(jnp.bfloat16)
    visible = lax.broadcasted_iota(jnp.int32, (ROWS, slots), 1) <= length
    out_row = lax.broadcasted_iota(jnp.int32, (ROWS, head), 0)
    attention = None
    for p in range(pairs):
        scores = lax.dot_general(
            own_queries, cache[p, :, :head], NT, preferred_element_type=jnp.float32
        ) * (1.0 / math.sqrt(head))
        scores = jnp.where(visible, scores, -1e30)
        peak = jnp.max(scores, axis=1, keepdims=True)
        weights = jnp.where(visible, jnp.exp(scores - peak), 0.0)
        denominator = jnp.sum(weights, axis=1, keepdims=True)
        weighted = jnp.dot(
            weights.astype(jnp.bfloat16), cache[p, :, head:], preferred_element_type=jnp.float32
        )
        result = weighted / denominator
        attention = result if p == 0 else jnp.where(out_row < p * share, attention, result)

    residual_rows[...] = jnp.zeros_like(residual_rows)
    for c in range(heads):
        at = pl.ds(pl.multiple_of(part * heads * LANES + c * LANES, LANES), LANES)
        residual_rows[c * seqs : (c + 1) * seqs, :] = residual[:, at].astype(jnp.float32)
    own_residual = residual_rows[pl.ds(seq, ROWS, stride=seqs), :]
    stream[seq] = (own_residual + attention).astype(jnp.bfloat16)

    sublane = lax.broadcasted_iota(jnp.int32, (seqs, LANES), 0)
    for k in range(routing.shape[0]):
        value = jnp.zeros((seqs, LANES), jnp.int32)
        for s in range(seqs):
            value = jnp.where(sublane == s, routing[k, s], value)
        routes[k] = value
    lane = lax.broadcasted_iota(jnp.int32, (seqs, LANES), 1)
    both = jnp.where(lane < LANES // 2, routes[0], routes[1])
    for to in range(groups):
        scaled[to, own_blocks] = both.astype(jnp.float32).astype(jnp.bfloat16)

    pl.semaphore_wait(barrier, tensors - 1 + jnp.where(lower, 0, chips))
    for i in sorted(range(1, seqs), key=lambda i: -min(i, seqs - i)):
        stream_copy(seq_peer(i)).start()

    @pl.when(lower)
    def _():
        for i in range(chips, groups):
            signal(group=i)

    @pl.when(jnp.logical_not(lower))
    def _():
        for i in range(chips):
            signal(group=i)

    keep = pltpu.make_async_copy(
        cache.at[:, pl.ds(pl.multiple_of(rank * span, span), span), :],
        cache_out.at[pl.ds(rank * pairs, pairs)],
        local_sem,
    )
    keep.start()
    for offset in offsets:
        if goes_first(*offset):
            cache_copy(tensor_peer(*offset)).start()
    for load in loads[6:]:
        load.wait()
    others = stream.at[pl.ds(0, seqs - 1)]
    remote(others, others, stream_send, stream_recv, tensor=rank).wait_recv()

    def scale_part(at):
        for c in range(heads):
            tile = raw[at, c].astype(jnp.float32)
            scaled[at * pieces + c // own_blocks, c % own_blocks] = (tile * gain[pl.ds(at * heads + c, 1), :]).astype(
                jnp.bfloat16
            )

    for k in range(seqs):
        stream_rows[k * ROWS : (k + 1) * ROWS, :] = stream[k].astype(jnp.float32)
    for c in range(heads):
        raw[part, c] = stream_rows[pl.ds(c, seqs, stride=ROWS), :].astype(jnp.bfloat16)
    each(parts, lambda i: raw_copy(part_peer(i)).start())
    for offset in offsets:
        if not goes_first(*offset):
            cache_copy(tensor_peer(*offset)).start()
    scale_part(part)

    @pl.when(lower)
    def _():
        pl.semaphore_wait(barrier, chips)
        signal(group=groups - 1 - mine)

    @pl.when(jnp.logical_not(lower))
    def _():
        pl.semaphore_wait(barrier, 1)

    def send_part(at):
        for piece in range(pieces):
            to = at * pieces + piece

            @pl.when(to != mine)
            def _():
                column_copy(to).start()

    send_part(part)
    own_columns = pltpu.make_async_copy(
        scaled.at[mine], columns.at[mine], column_recv.at[batch]
    )
    other_parts = raw.at[pl.ds(0, parts - 1)]
    remote(other_parts, other_parts, raw_send, raw_recv, group=mine).wait_recv()
    for i in range(1, parts):
        scale_part(part_peer(i))
    for i in range(1, parts):
        send_part(part_peer(i))
    own_columns.start()

    def choose(to, target, at):
        rows = pl.ds(pl.multiple_of(to * seqs, seqs), seqs)
        both = columns[to, own_blocks].astype(jnp.float32)
        swapped = pltpu.roll(both, LANES // 2, 1)
        for k in range(2):
            near, far = (both, swapped) if k == 0 else (swapped, both)
            route = jnp.where(lane < LANES // 2, near, far)
            route = jnp.concatenate([route] * (hidden // LANES), axis=1)
            for q, source in enumerate((gate_all, up_all)):
                value = source[0, rows, :]
                for e in range(1, experts):
                    value = jnp.where(route == float(e), source[e, rows, :], value)
                target[at, 2 * k + q] = value.astype(target.dtype)

    def pair_copy(b):
        first, last = batches[b]
        at = pl.ds(first, last - first)
        return remote(
            pair_out.at[at],
            pair_in.at[at],
            pair_send.at[b],
            pair_recv.at[b],
            group=2 * chip + 1 - core,
        )

    def expert_batch(b):
        first, last = batches[b]
        count = last - first
        some = columns.at[pl.ds(2 * first, 2 * count)]
        remote(some, some, column_send, column_recv.at[b], group=mine).wait_recv()
        rows = pl.ds(2 * first * seqs, 2 * count * seqs)
        for c in range(own_blocks):
            tokens[rows, c * LANES : (c + 1) * LANES] = (
                columns[pl.ds(2 * first, 2 * count), c]
                .astype(jnp.float32)
                .reshape(2 * count * seqs, LANES)
                .astype(jnp.bfloat16)
            )
        for e in range(experts):
            gate_all[e, rows, :] = jnp.dot(
                tokens[rows, :], gate_w[e], preferred_element_type=jnp.float32
            )
            up_all[e, rows, :] = jnp.dot(
                tokens[rows, :], up_w[e], preferred_element_type=jnp.float32
            )

        def for_pair(i, carry):
            choose(2 * i + 1 - core, pair_out, i)
            return carry

        def for_own(i, carry):
            choose(2 * i + core, pair_own, i)
            return carry

        lax.fori_loop(first, last, for_pair, 0)
        pair_copy(b).start()
        lax.fori_loop(first, last, for_own, 0)
        pair_copy(b).wait_recv()
        order = list(range(first, last))

        def send_sum(to):
            @pl.when(to != chip)
            def _():
                sum_copy(to).start()

        for n, to in enumerate(order):
            partial[to] = (pair_own[to] + pair_in[to].astype(jnp.float32)).astype(jnp.bfloat16)
            if n:
                send_sum(order[n - 1])
        send_sum(order[-1])

    expert_batch(0)

    total = jnp.zeros((seqs, LANES), jnp.float32)
    for c in range(blocks):
        value = raw[c // heads, c % heads]
        updated_out[:, c * LANES : (c + 1) * LANES] = value
        value = value.astype(jnp.float32)
        total = total + value * value
    scale = lax.rsqrt(jnp.sum(total, axis=1, keepdims=True) / cols + 1e-05)
    for c in range(blocks):
        value = raw[c // heads, c % heads].astype(jnp.float32)
        normed[:, c * LANES : (c + 1) * LANES] = (value * scale * gain[c : c + 1, :]).astype(
            jnp.bfloat16
        )
    logits = lax.dot_general(normed[...], router[...], NT, preferred_element_type=jnp.float32)
    expert_id = lax.broadcasted_iota(jnp.int32, (seqs, experts), 1)
    chosen = [
        jnp.sum(
            jnp.where(routes[k][:, :1] == expert_id, logits, 0.0), axis=1, keepdims=True
        )
        for k in range(2)
    ]
    gate_weights = [
        1.0 / (1.0 + jnp.exp(chosen[1] - chosen[0])),
        1.0 / (1.0 + jnp.exp(chosen[0] - chosen[1])),
    ]

    expert_batch(1)
    arrived[chip] = partial[chip]
    other_sums = arrived.at[pl.ds(0, chips - 1)]
    remote(other_sums, other_sums, sum_send, sum_recv, group=mine).wait_recv()
    units = []
    for k in range(2):
        sums = []
        for q in range(2):
            value = arrived[0, 2 * k + q].astype(jnp.float32)
            for s in range(1, chips):
                value = value + arrived[s, 2 * k + q].astype(jnp.float32)
            sums.append(value * scale)
        silu = sums[0] / (1.0 + jnp.exp(-sums[0]))
        units.append(gate_weights[k] * silu * sums[1])
    for s in range(seqs):
        hidden_out[s] = jnp.concatenate([unit[s : s + 1] for unit in units], axis=0).astype(
            jnp.bfloat16
        )

    remote(others, others, stream_send, stream_recv, tensor=rank).wait_send()
    remote(other_parts, other_parts, raw_send, raw_recv, group=mine).wait_send()
    for b in range(2):
        pair_copy(b).wait_send()
    remote(other_sums, other_sums, sum_send, sum_recv, group=mine).wait_send()
    most = columns.at[pl.ds(0, groups - 1)]
    remote(most, most, column_send, column_recv.at[0], group=mine).wait_send()

    most_cache = cache_out.at[pl.ds(0, (tensors - 1) * pairs)]
    remote(most_cache, most_cache, cache_send, cache_recv, tensor=rank).wait_send()
    keep.wait()
    remote(most_cache, most_cache, cache_send, cache_recv, tensor=rank).wait_recv()


def write_out(updated, hidden_units, cache, updated_hbm, hidden_hbm, cache_hbm, sems):
    copies = [
        pltpu.make_async_copy(source, target, sems.at[k])
        for k, (source, target) in enumerate(
            ((cache, cache_hbm), (updated, updated_hbm), (hidden_units, hidden_hbm))
        )
    ]
    for copy in copies:
        copy.start()
    for copy in copies:
        copy.wait()


def body(
    groups,
    tensors,
    key_value_cache,
    queries,
    fresh_key_value,
    lengths,
    residual,
    norm_gain,
    router_weight,
    routing,
    expert_gate,
    expert_up,
):
    pairs, slots, width = key_value_cache.shape
    seqs, q_heads, head = queries.shape
    kv_heads = fresh_key_value.shape[1]
    cols = residual.shape[1]
    experts, own_cols, hidden = expert_gate.shape
    span = slots // tensors
    parts = tensors // seqs
    heads = cols // parts // head
    bf16, f32, i32 = jnp.bfloat16, jnp.float32, jnp.int32
    dma = pltpu.SemaphoreType.DMA
    hbm = pl.BlockSpec(memory_space=pltpu.HBM)
    vmem = pl.BlockSpec(memory_space=pltpu.VMEM)
    updated, hidden_units, new_cache = pl.pallas_call(
        functools.partial(kernel, (groups, tensors, span)),
        out_shape=(
            pltpu.VMEM((seqs, cols), bf16),
            pltpu.VMEM((seqs, 2, hidden), bf16),
            pltpu.VMEM((seqs * kv_heads, span, width), bf16),
        ),
        in_specs=[hbm] * 10,
        out_specs=(vmem, vmem, vmem),
        scratch_shapes=[
            pltpu.SMEM((seqs,), i32),
            pltpu.SMEM((2, seqs), i32),
            pltpu.VMEM((pairs, slots, width), bf16),
            pltpu.VMEM((q_heads, head), bf16),
            pltpu.VMEM((kv_heads, width), bf16),
            pltpu.VMEM((seqs, cols), bf16),
            pltpu.VMEM((cols // LANES, LANES), f32),
            pltpu.VMEM((experts, cols), bf16),
            pltpu.VMEM(expert_gate.shape, bf16),
            pltpu.VMEM(expert_up.shape, bf16),
            pltpu.VMEM(((ROWS + 1) * seqs, LANES), f32),
            pltpu.VMEM((seqs, ROWS, LANES), bf16),
            pltpu.VMEM((seqs * ROWS, LANES), f32),
            pltpu.VMEM((parts, heads, seqs, LANES), bf16),
            pltpu.VMEM((groups, own_cols // LANES + 1, seqs, LANES), bf16),
            pltpu.VMEM((seqs, cols), bf16),
            pltpu.VMEM((groups, own_cols // LANES + 1, seqs, LANES), bf16),
            pltpu.VMEM((groups * seqs, own_cols), bf16),
            pltpu.VMEM((2, seqs, LANES), i32),
            pltpu.VMEM((experts, groups * seqs, hidden), f32),
            pltpu.VMEM((experts, groups * seqs, hidden), f32),
            pltpu.VMEM((groups // 2, 4, seqs, hidden), bf16),
            pltpu.VMEM((groups // 2, 4, seqs, hidden), bf16),
            pltpu.VMEM((groups // 2, 4, seqs, hidden), f32),
            pltpu.VMEM((groups // 2, 4, seqs, hidden), bf16),
            pltpu.VMEM((groups // 2, 4, seqs, hidden), bf16),
            dma((10,)),
        ]
        + [dma(())] * 8
        + [dma((2,))] * 3
        + [dma(())] * 2,
        compiler_params=pltpu.CompilerParams(
            collective_id=0, has_side_effects=True
        ),
    )(
        lengths,
        routing.T,
        key_value_cache,
        queries,
        fresh_key_value,
        residual,
        norm_gain.reshape(cols // LANES, LANES),
        router_weight.T,
        expert_gate,
        expert_up,
    )
    updated, hidden_units, new_cache = pl.pallas_call(
        write_out,
        out_shape=(
            jax.ShapeDtypeStruct(updated.shape, bf16),
            jax.ShapeDtypeStruct(hidden_units.shape, bf16),
            jax.ShapeDtypeStruct(new_cache.shape, bf16),
        ),
        in_specs=[vmem] * 3,
        out_specs=(hbm,) * 3,
        scratch_shapes=[dma((3,))],
        compiler_params=pltpu.CompilerParams(vmem_limit_bytes=4 << 20),
    )(updated, hidden_units, new_cache)
    return (
        updated,
        hidden_units,
        new_cache.reshape(seqs, kv_heads, span, width),
    )


def solution(mesh):
    in_specs = (
        P(("group", "tensor"), None, None),
        P("group", None, None),
        P("group", None, None),
        P("group"),
        P("group", None),
        P(),
        P(),
        P("group", None),
        P(None, "group", "tensor"),
        P(None, "group", "tensor"),
    )
    out_specs = (P("group", None), P("group", None, "tensor"), P("group", None, "tensor", None))
    return jax.shard_map(
        functools.partial(body, mesh.shape["group"], mesh.shape["tensor"]),
        mesh=mesh,
        in_specs=in_specs,
        out_specs=out_specs,
        check_vma=False,
    )
```

```python
import functools
import math

import jax
import jax.numpy as jnp
from jax import lax
from jax.experimental import pallas as pl
from jax.experimental.pallas import tpu as pltpu
from jax.sharding import PartitionSpec as P

MESH = pl.DeviceIdType.MESH
LANES = 128
ROWS = 16
NT = (((1,), (1,)), ((), ()))


EARLY = 3


def goes_first(down, along):
    return along == 0 or down in (0, 1, 7) or (down in (2, 6) and along == 2)


def kernel(
    dims,
    lengths_hbm,
    routing_hbm,
    cache_hbm,
    queries_hbm,
    fresh_hbm,
    residual_hbm,
    gain_hbm,
    router_hbm,
    gate_hbm,
    up_hbm,
    updated_out,
    hidden_out,
    cache_out,
    lengths,
    routing,
    cache,
    queries,
    fresh,
    residual,
    gain,
    router,
    gate_w,
    up_w,
    residual_rows,
    stream,
    stream_rows,
    raw,
    scaled,
    normed,
    columns,
    tokens,
    routes,
    gate_all,
    up_all,
    pair_out,
    pair_in,
    pair_own,
    partial,
    arrived,
    load_sem,
    local_sem,
    stream_send,
    stream_recv,
    raw_send,
    raw_recv,
    cache_send,
    cache_recv,
    column_send,
    column_recv,
    pair_send,
    pair_recv,
    sum_send,
    sum_recv,
):
    groups, tensors, span = dims
    mine = lax.axis_index("group")
    rank = lax.axis_index("tensor")
    pairs, slots, width = cache.shape
    head = width // 2
    seqs, cols = updated_out.shape
    parts = tensors // seqs
    seq = rank // parts
    part = lax.rem(rank, parts)
    heads = cols // parts // head
    share = heads // pairs
    blocks = cols // LANES
    own_blocks = blocks // groups
    pieces = groups // parts
    experts = gate_w.shape[0]
    hidden = gate_w.shape[2]
    chips = groups // 2
    chip = mine // 2
    core = lax.rem(mine, 2)
    lower = mine < chips
    batches = ((0, EARLY), (EARLY, chips))
    batch = jnp.where(chip < EARLY, 0, 1)

    def group_peer(i):
        return lax.rem(mine + i, groups)

    def seq_peer(i):
        return lax.rem(seq + i, seqs)

    def part_peer(i):
        return lax.rem(part + i, parts)

    def chip_peer(i):
        return lax.rem(chip + i, chips)

    def tensor_peer(down, along):
        return lax.rem(seq + down, seqs) * parts + lax.rem(part + along, parts)

    offsets = sorted(
        ((down, along) for down in range(seqs) for along in range(parts) if down or along),
        key=lambda o: -min(o[0], seqs - o[0]) - min(o[1], parts - o[1]),
    )

    def remote(source, target, send, recv, **to):
        return pltpu.make_async_remote_copy(
            src_ref=source,
            dst_ref=target,
            send_sem=send,
            recv_sem=recv,
            device_id=to,
            device_id_type=MESH,
        )

    def cache_copy(to):
        return remote(
            cache.at[:, pl.ds(pl.multiple_of(to * span, span), span), :],
            cache_out.at[pl.ds(rank * pairs, pairs)],
            cache_send,
            cache_recv,
            tensor=to,
        )

    def stream_copy(to):
        return remote(
            stream.at[seq], stream.at[seq], stream_send, stream_recv, tensor=to * parts + part
        )

    def raw_copy(to):
        return remote(raw.at[part], raw.at[part], raw_send, raw_recv, tensor=seq * parts + to)

    def column_copy(to):
        return remote(
            scaled.at[to],
            columns.at[mine],
            column_send,
            column_recv.at[batch],
            group=to,
        )

    def sum_copy(to):
        return remote(
            partial.at[to], arrived.at[chip], sum_send, sum_recv, group=2 * to + core
        )

    def signal(**to):
        pl.semaphore_signal(barrier, inc=1, device_id=to, device_id_type=MESH)

    def each(count, step):
        def go(i, carry):
            step(i)
            return carry

        lax.fori_loop(1, count, go, 0)

    barrier = pltpu.get_barrier_semaphore()
    for offset in offsets:
        signal(tensor=tensor_peer(*offset))

    loads = [
        pltpu.make_async_copy(source, target, load_sem.at[k])
        for k, (source, target) in enumerate(
            (
                (cache_hbm, cache),
                (lengths_hbm, lengths),
                (queries_hbm.at[seq], queries),
                (fresh_hbm.at[seq], fresh),
                (residual_hbm, residual),
                (routing_hbm, routing),
                (gain_hbm, gain),
                (router_hbm, router),
                (gate_hbm, gate_w),
                (up_hbm, up_w),
            )
        )
    ]
    for load in loads[:6]:
        load.start()

    for load in loads[:6]:
        load.wait()
    for load in loads[6:]:
        load.start()

    length = lengths[seq]
    fresh_rows = fresh[...].astype(jnp.float32)
    row_id = lax.broadcasted_iota(jnp.int32, fresh_rows.shape, 0)
    chunk = 128
    for p in range(pairs):
        own_row = jnp.sum(
            jnp.where(row_id == part * pairs + p, fresh_rows, 0.0), axis=0, keepdims=True
        )

        def place(c, carry, p=p, own_row=own_row):
            at = pl.ds(pl.multiple_of(c * chunk, chunk), chunk)
            slot_id = lax.broadcasted_iota(jnp.int32, (chunk, width), 0) + c * chunk
            cache[p, at, :] = jnp.where(
                slot_id == length, own_row, cache[p, at, :].astype(jnp.float32)
            ).astype(jnp.bfloat16)
            return carry

        lax.fori_loop(0, slots // chunk, place, 0)

    pick = (
        lax.broadcasted_iota(jnp.int32, (ROWS, queries.shape[0]), 1)
        == lax.broadcasted_iota(jnp.int32, (ROWS, queries.shape[0]), 0) + part * heads
    )
    own_queries = jnp.dot(
        pick.astype(jnp.float32).astype(jnp.bfloat16),
        queries[...],
        preferred_element_type=jnp.float32,
    ).astype(jnp.bfloat16)
    visible = lax.broadcasted_iota(jnp.int32, (ROWS, slots), 1) <= length
    out_row = lax.broadcasted_iota(jnp.int32, (ROWS, head), 0)
    attention = None
    for p in range(pairs):
        scores = lax.dot_general(
            own_queries, cache[p, :, :head], NT, preferred_element_type=jnp.float32
        ) * (1.0 / math.sqrt(head))
        scores = jnp.where(visible, scores, -1e30)
        peak = jnp.max(scores, axis=1, keepdims=True)
        weights = jnp.where(visible, jnp.exp(scores - peak), 0.0)
        denominator = jnp.sum(weights, axis=1, keepdims=True)
        weighted = jnp.dot(
            weights.astype(jnp.bfloat16), cache[p, :, head:], preferred_element_type=jnp.float32
        )
        result = weighted / denominator
        attention = result if p == 0 else jnp.where(out_row < p * share, attention, result)

    residual_rows[...] = jnp.zeros_like(residual_rows)
    for c in range(heads):
        at = pl.ds(pl.multiple_of(part * heads * LANES + c * LANES, LANES), LANES)
        residual_rows[c * seqs : (c + 1) * seqs, :] = residual[:, at].astype(jnp.float32)
    own_residual = residual_rows[pl.ds(seq, ROWS, stride=seqs), :]
    stream[seq] = (own_residual + attention).astype(jnp.bfloat16)

    sublane = lax.broadcasted_iota(jnp.int32, (seqs, LANES), 0)
    for k in range(routing.shape[0]):
        value = jnp.zeros((seqs, LANES), jnp.int32)
        for s in range(seqs):
            value = jnp.where(sublane == s, routing[k, s], value)
        routes[k] = value
    lane = lax.broadcasted_iota(jnp.int32, (seqs, LANES), 1)
    both = jnp.where(lane < LANES // 2, routes[0], routes[1])
    for to in range(groups):
        scaled[to, own_blocks] = both.astype(jnp.float32).astype(jnp.bfloat16)

    pl.semaphore_wait(barrier, tensors - 1 + jnp.where(lower, 0, chips))
    for i in sorted(range(1, seqs), key=lambda i: -min(i, seqs - i)):
        stream_copy(seq_peer(i)).start()

    @pl.when(lower)
    def _():
        for i in range(chips, groups):
            signal(group=i)

    @pl.when(jnp.logical_not(lower))
    def _():
        for i in range(chips):
            signal(group=i)

    keep = pltpu.make_async_copy(
        cache.at[:, pl.ds(pl.multiple_of(rank * span, span), span), :],
        cache_out.at[pl.ds(rank * pairs, pairs)],
        local_sem,
    )
    keep.start()
    for offset in offsets:
        if goes_first(*offset):
            cache_copy(tensor_peer(*offset)).start()
    for load in loads[6:]:
        load.wait()
    others = stream.at[pl.ds(0, seqs - 1)]
    remote(others, others, stream_send, stream_recv, tensor=rank).wait_recv()

    def scale_part(at):
        for c in range(heads):
            tile = raw[at, c].astype(jnp.float32)
            scaled[at * pieces + c // own_blocks, c % own_blocks] = (tile * gain[pl.ds(at * heads + c, 1), :]).astype(
                jnp.bfloat16
            )

    for k in range(seqs):
        stream_rows[k * ROWS : (k + 1) * ROWS, :] = stream[k].astype(jnp.float32)
    for c in range(heads):
        raw[part, c] = stream_rows[pl.ds(c, seqs, stride=ROWS), :].astype(jnp.bfloat16)
    each(parts, lambda i: raw_copy(part_peer(i)).start())
    for offset in offsets:
        if not goes_first(*offset):
            cache_copy(tensor_peer(*offset)).start()
    scale_part(part)

    @pl.when(lower)
    def _():
        pl.semaphore_wait(barrier, chips)
        signal(group=groups - 1 - mine)

    @pl.when(jnp.logical_not(lower))
    def _():
        pl.semaphore_wait(barrier, 1)

    def send_part(at):
        for piece in range(pieces):
            to = at * pieces + piece

            @pl.when(to != mine)
            def _():
                column_copy(to).start()

    send_part(part)
    own_columns = pltpu.make_async_copy(
        scaled.at[mine], columns.at[mine], column_recv.at[batch]
    )
    other_parts = raw.at[pl.ds(0, parts - 1)]
    remote(other_parts, other_parts, raw_send, raw_recv, group=mine).wait_recv()
    for i in range(1, parts):
        scale_part(part_peer(i))
    for i in range(1, parts):
        send_part(part_peer(i))
    own_columns.start()

    def choose(to, target, at):
        rows = pl.ds(pl.multiple_of(to * seqs, seqs), seqs)
        both = columns[to, own_blocks].astype(jnp.float32)
        swapped = pltpu.roll(both, LANES // 2, 1)
        for k in range(2):
            near, far = (both, swapped) if k == 0 else (swapped, both)
            route = jnp.where(lane < LANES // 2, near, far)
            route = jnp.concatenate([route] * (hidden // LANES), axis=1)
            for q, source in enumerate((gate_all, up_all)):
                value = source[0, rows, :]
                for e in range(1, experts):
                    value = jnp.where(route == float(e), source[e, rows, :], value)
                target[at, 2 * k + q] = value.astype(target.dtype)

    def pair_copy(b):
        first, last = batches[b]
        at = pl.ds(first, last - first)
        return remote(
            pair_out.at[at],
            pair_in.at[at],
            pair_send.at[b],
            pair_recv.at[b],
            group=2 * chip + 1 - core,
        )

    def expert_batch(b):
        first, last = batches[b]
        count = last - first
        some = columns.at[pl.ds(2 * first, 2 * count)]
        remote(some, some, column_send, column_recv.at[b], group=mine).wait_recv()
        rows = pl.ds(2 * first * seqs, 2 * count * seqs)
        for c in range(own_blocks):
            tokens[rows, c * LANES : (c + 1) * LANES] = (
                columns[pl.ds(2 * first, 2 * count), c]
                .astype(jnp.float32)
                .reshape(2 * count * seqs, LANES)
                .astype(jnp.bfloat16)
            )
        for e in range(experts):
            gate_all[e, rows, :] = jnp.dot(
                tokens[rows, :], gate_w[e], preferred_element_type=jnp.float32
            )
            up_all[e, rows, :] = jnp.dot(
                tokens[rows, :], up_w[e], preferred_element_type=jnp.float32
            )

        def for_pair(i, carry):
            choose(2 * i + 1 - core, pair_out, i)
            return carry

        def for_own(i, carry):
            choose(2 * i + core, pair_own, i)
            return carry

        lax.fori_loop(first, last, for_pair, 0)
        pair_copy(b).start()
        lax.fori_loop(first, last, for_own, 0)
        pair_copy(b).wait_recv()
        order = list(range(first, last))

        def send_sum(to):
            @pl.when(to != chip)
            def _():
                sum_copy(to).start()

        for n, to in enumerate(order):
            partial[to] = (pair_own[to] + pair_in[to].astype(jnp.float32)).astype(jnp.bfloat16)
            if n:
                send_sum(order[n - 1])
        send_sum(order[-1])

    expert_batch(0)

    total = jnp.zeros((seqs, LANES), jnp.float32)
    for c in range(blocks):
        value = raw[c // heads, c % heads]
        updated_out[:, c * LANES : (c + 1) * LANES] = value
        value = value.astype(jnp.float32)
        total = total + value * value
    scale = lax.rsqrt(jnp.sum(total, axis=1, keepdims=True) / cols + 1e-05)
    for c in range(blocks):
        value = raw[c // heads, c % heads].astype(jnp.float32)
        normed[:, c * LANES : (c + 1) * LANES] = (value * scale * gain[c : c + 1, :]).astype(
            jnp.bfloat16
        )
    logits = lax.dot_general(normed[...], router[...], NT, preferred_element_type=jnp.float32)
    expert_id = lax.broadcasted_iota(jnp.int32, (seqs, experts), 1)
    chosen = [
        jnp.sum(
            jnp.where(routes[k][:, :1] == expert_id, logits, 0.0), axis=1, keepdims=True
        )
        for k in range(2)
    ]
    gate_weights = [
        1.0 / (1.0 + jnp.exp(chosen[1] - chosen[0])),
        1.0 / (1.0 + jnp.exp(chosen[0] - chosen[1])),
    ]

    expert_batch(1)
    arrived[chip] = partial[chip]
    other_sums = arrived.at[pl.ds(0, chips - 1)]
    remote(other_sums, other_sums, sum_send, sum_recv, group=mine).wait_recv()
    units = []
    for k in range(2):
        sums = []
        for q in range(2):
            value = arrived[0, 2 * k + q].astype(jnp.float32)
            for s in range(1, chips):
                value = value + arrived[s, 2 * k + q].astype(jnp.float32)
            sums.append(value * scale)
        silu = sums[0] / (1.0 + jnp.exp(-sums[0]))
        units.append(gate_weights[k] * silu * sums[1])
    for s in range(seqs):
        hidden_out[s] = jnp.concatenate([unit[s : s + 1] for unit in units], axis=0).astype(
            jnp.bfloat16
        )

    remote(others, others, stream_send, stream_recv, tensor=rank).wait_send()
    remote(other_parts, other_parts, raw_send, raw_recv, group=mine).wait_send()
    for b in range(2):
        pair_copy(b).wait_send()
    remote(other_sums, other_sums, sum_send, sum_recv, group=mine).wait_send()
    most = columns.at[pl.ds(0, groups - 1)]
    remote(most, most, column_send, column_recv.at[0], group=mine).wait_send()

    most_cache = cache_out.at[pl.ds(0, (tensors - 1) * pairs)]
    remote(most_cache, most_cache, cache_send, cache_recv, tensor=rank).wait_send()
    keep.wait()
    remote(most_cache, most_cache, cache_send, cache_recv, tensor=rank).wait_recv()


def write_out(updated, hidden_units, cache, updated_hbm, hidden_hbm, cache_hbm, sems):
    copies = [
        pltpu.make_async_copy(source, target, sems.at[k])
        for k, (source, target) in enumerate(
            ((cache, cache_hbm), (updated, updated_hbm), (hidden_units, hidden_hbm))
        )
    ]
    for copy in copies:
        copy.start()
    for copy in copies:
        copy.wait()


def body(
    groups,
    tensors,
    key_value_cache,
    queries,
    fresh_key_value,
    lengths,
    residual,
    norm_gain,
    router_weight,
    routing,
    expert_gate,
    expert_up,
):
    pairs, slots, width = key_value_cache.shape
    seqs, q_heads, head = queries.shape
    kv_heads = fresh_key_value.shape[1]
    cols = residual.shape[1]
    experts, own_cols, hidden = expert_gate.shape
    span = slots // tensors
    parts = tensors // seqs
    heads = cols // parts // head
    bf16, f32, i32 = jnp.bfloat16, jnp.float32, jnp.int32
    dma = pltpu.SemaphoreType.DMA
    hbm = pl.BlockSpec(memory_space=pltpu.HBM)
    vmem = pl.BlockSpec(memory_space=pltpu.VMEM)
    updated, hidden_units, new_cache = pl.pallas_call(
        functools.partial(kernel, (groups, tensors, span)),
        out_shape=(
            pltpu.VMEM((seqs, cols), bf16),
            pltpu.VMEM((seqs, 2, hidden), bf16),
            pltpu.VMEM((seqs * kv_heads, span, width), bf16),
        ),
        in_specs=[hbm] * 10,
        out_specs=(vmem, vmem, vmem),
        scratch_shapes=[
            pltpu.SMEM((seqs,), i32),
            pltpu.SMEM((2, seqs), i32),
            pltpu.VMEM((pairs, slots, width), bf16),
            pltpu.VMEM((q_heads, head), bf16),
            pltpu.VMEM((kv_heads, width), bf16),
            pltpu.VMEM((seqs, cols), bf16),
            pltpu.VMEM((cols // LANES, LANES), f32),
            pltpu.VMEM((experts, cols), bf16),
            pltpu.VMEM(expert_gate.shape, bf16),
            pltpu.VMEM(expert_up.shape, bf16),
            pltpu.VMEM(((ROWS + 1) * seqs, LANES), f32),
            pltpu.VMEM((seqs, ROWS, LANES), bf16),
            pltpu.VMEM((seqs * ROWS, LANES), f32),
            pltpu.VMEM((parts, heads, seqs, LANES), bf16),
            pltpu.VMEM((groups, own_cols // LANES + 1, seqs, LANES), bf16),
            pltpu.VMEM((seqs, cols), bf16),
            pltpu.VMEM((groups, own_cols // LANES + 1, seqs, LANES), bf16),
            pltpu.VMEM((groups * seqs, own_cols), bf16),
            pltpu.VMEM((2, seqs, LANES), i32),
            pltpu.VMEM((experts, groups * seqs, hidden), f32),
            pltpu.VMEM((experts, groups * seqs, hidden), f32),
            pltpu.VMEM((groups // 2, 4, seqs, hidden), bf16),
            pltpu.VMEM((groups // 2, 4, seqs, hidden), bf16),
            pltpu.VMEM((groups // 2, 4, seqs, hidden), f32),
            pltpu.VMEM((groups // 2, 4, seqs, hidden), bf16),
            pltpu.VMEM((groups // 2, 4, seqs, hidden), bf16),
            dma((10,)),
        ]
        + [dma(())] * 8
        + [dma((2,))] * 3
        + [dma(())] * 2,
        compiler_params=pltpu.CompilerParams(
            collective_id=0, has_side_effects=True
        ),
    )(
        lengths,
        routing.T,
        key_value_cache,
        queries,
        fresh_key_value,
        residual,
        norm_gain.reshape(cols // LANES, LANES),
        router_weight.T,
        expert_gate,
        expert_up,
    )
    updated, hidden_units, new_cache = pl.pallas_call(
        write_out,
        out_shape=(
            jax.ShapeDtypeStruct(updated.shape, bf16),
            jax.ShapeDtypeStruct(hidden_units.shape, bf16),
            jax.ShapeDtypeStruct(new_cache.shape, bf16),
        ),
        in_specs=[vmem] * 3,
        out_specs=(hbm,) * 3,
        scratch_shapes=[dma((3,))],
        compiler_params=pltpu.CompilerParams(vmem_limit_bytes=4 << 20),
    )(updated, hidden_units, new_cache)
    return (
        updated,
        hidden_units,
        new_cache.reshape(seqs, kv_heads, span, width),
    )


def solution(mesh):
    in_specs = (
        P(("group", "tensor"), None, None),
        P("group", None, None),
        P("group", None, None),
        P("group"),
        P("group", None),
        P(),
        P(),
        P("group", None),
        P(None, "group", "tensor"),
        P(None, "group", "tensor"),
    )
    out_specs = (P("group", None), P("group", None, "tensor"), P("group", None, "tensor", None))
    return jax.shard_map(
        functools.partial(body, mesh.shape["group"], mesh.shape["tensor"]),
        mesh=mesh,
        in_specs=in_specs,
        out_specs=out_specs,
        check_vma=False,
    )
```
